128 devices in a mesh: pole: 4 (over x_hi, core), row: 4 (over y), col: 8 (over x_lo, z).
Axes of the slice: x: 4 (x_hi: 2, x_lo: 2; x = x_hi * 2 + x_lo), y: 4, z: 4, core: 2. Of those that a mesh axis runs over, the one named last changes fastest.
Arguments:
- inverse: bfloat16 [4, 2, 4096, 4096], P('pole', None, 'row', 'col'), may hold values from -0.0625 to 0.0625
- factor: bfloat16 [4, 1, 2048, 1024], P('pole', None, ('row', 'col')), may hold values from -1.796875 to 1.796875
- dinv: float32 [512, 4, 1, 2, 512], P(('row', 'col'), 'pole'), may hold values from -6 to 6
- ancestors: int32 [1, 16], replicated, may hold values from 0 to 31, as said below
- owner: int32 [2048, 1], P(('row', 'col')), may hold values from 0 to 127; in each aligned block of 64 rows (0 to 63, 64 to 127, ...) at most 2 rows name the same one
- weight_table: float32 [2, 16], replicated, may hold values from -4 to 4
- pole_slot: int32 [4], P('pole'), may hold values from 0 to 15
Outputs:
- inverse_column: float32 [4096, 4, 1, 2, 512], P(('row', 'col'), 'pole')
- diag_inverse: float32 [512, 4, 1, 2, 512], P(('row', 'col'), 'pole')
- density_diag: float32 [512, 1, 512], P(('row', 'col'))
- tile_density: float32 [128, 8, 128], P(('pole', 'row', 'col'))
The draws below stay inside these ranges and needn't reach their ends.
Inputs may be any that keep to these rules, and one draw needn't show every extreme that they name: `ancestors`: each row lists 16 distinct block numbers in increasing order. In the rows of one device (64 rows of owner) no tile is named more than 2 times.
All inputs are finite; a program needn't handle non-finite values.
Results may differ from the reference program's by a relative error of at most 0.0028.
Values may be sent and summed in bfloat16 or wider, within the bound.
A program may use at most 64 MiB of HBM per device.

```python
import math
import jax
import jax.numpy as jnp
import numpy as np
from jax import lax

A = 4096
S = 512
SN = 1
BS = 128
NSEL = 16
BR = 8
BC = 128
NWEIGHT = 16
POLES = 4
TILES = 128
NBLOCKS = 2048
HB = 64
CAP = 2


def draw_ancestors(key, part):
    listed = []
    for supernode in range(SN):
        shuffled = jax.random.permutation(jax.random.fold_in(key, 7919 + supernode), A // BS)
        listed.append(jnp.sort(shuffled[:NSEL]))
    return jnp.stack(listed).astype(jnp.int32)


def set_ends(result, own_key, low, top_value):
    dims = result.shape
    place = [jax.random.randint(jax.random.fold_in(own_key, axis), (), 0, dims[axis]) for axis in range(len(dims))]
    result = result.at[tuple(place)].set(low)
    longest = dims.index(max(dims))
    place[longest] = (place[longest] + 1) % dims[longest]
    return result.at[tuple(place)].set(top_value)


def level_of(key, dims, cuts, smallest, high):
    factor_of = 1.0
    for axis_at, shards_of in cuts:
        steps = jax.random.uniform(jax.random.fold_in(jax.random.fold_in(key, 6), axis_at), (shards_of,), jnp.float32, smallest / len(cuts), high / len(cuts))
        factor_of = factor_of * jnp.repeat(jnp.exp(steps), dims[axis_at] // shards_of).reshape((-1,) + (1,) * (len(dims) - 1 - axis_at))
    return factor_of


def routed_block(stream_key, own, number, rows, number_of, top, limit, skew):
    sequence = jax.random.permutation(stream_key, number_of)
    crowded, usual = load_shares(number_of, rows * top, limit, skew, True), load_shares(number_of, rows * top, limit, skew, False)
    places = jnp.arange(number_of)

    def named(lengths, turn):
        used = int((lengths > 0).sum())
        fixed = max(1, used // 4)
        moved = fixed + (places - fixed + turn * (used - fixed)) % max(1, number_of - fixed)
        return jnp.zeros((number_of,), jnp.int32).at[sequence[jnp.where(places < fixed, places, moved)]].set(jnp.asarray(lengths, jnp.int32))

    lengths = jnp.where(number % 4 == 0, named(crowded, number // 4), named(usual, number - number // 4 - 1))
    mixed = jax.random.permutation(jax.random.fold_in(own, 3), number_of)
    giver, taker = mixed[0:number_of // 2 * 2:2], mixed[1:number_of // 2 * 2:2]
    margin = jnp.minimum(lengths[giver] - 1, limit - lengths[taker]) // 2
    margin = jnp.where((giver == sequence[0]) | (taker == sequence[0]) | (lengths[taker] == 0), 0, jnp.maximum(margin, 0))
    moved = jax.random.randint(jax.random.fold_in(own, 4), (number_of // 2,), 0, 1 << 20) % (margin + 1)
    lengths = lengths.at[giver].add(-moved).at[taker].add(moved)
    labels = jnp.searchsorted(jnp.cumsum(lengths), jnp.arange(rows * top), side="right").astype(jnp.int32)
    listing = labels.reshape(top, rows).T
    listing = listing[jax.random.permutation(jax.random.fold_in(own, 1), rows)]
    turn = jax.random.randint(jax.random.fold_in(own, 2), (rows, 1), 0, top)
    return jnp.take_along_axis(listing, (jnp.arange(top)[None, :] + turn) % top, axis=1)


def load_shares(count, total, most, slope, full):
    loads = [(1 << 20) // math.isqrt(standing ** slope) + 1 for standing in range(1, count + 1)]
    largest = most if full else min(most, max(-(-total // count), total * loads[0] // sum(loads)))
    least = 1 if total - largest >= count - 1 else 0
    given, rest = [largest] + [least] * (count - 1), total - largest - least * (count - 1)
    while rest > 0:
        free = [i for i in range(1, count) if given[i] < largest] or [i for i in range(1, count) if given[i] < most]
        whole, budget = sum([loads[i] for i in free]), rest
        for i in free:
            addition = min(most - given[i], max(1, budget * loads[i] // whole), rest)
            given[i] = given[i] + addition
            rest = rest - addition
    return np.array(given)


def noise(own_key, shape, spread, limit, split=(), kind=jnp.bfloat16):
    loudness = level_of(own_key, shape, split, -0.22, 0.18) if split else 1.0
    drawn = jax.random.normal(own_key, shape, jnp.float32) * spread * loudness
    return jnp.minimum(jnp.maximum(drawn, -limit), limit).astype(kind)


def setup_inputs(seed: int = 0) -> dict:
    streams_of = jax.random.split(jax.random.key(seed), 8)
    inverse = noise(streams_of[0], (POLES, 2, A, A), (2 * A) ** -0.5, 0.0625, ((0, 4), (2, 4), (3, 8)))
    factor = noise(streams_of[1], (POLES, SN, NSEL * BS, 2 * S), 0.3, 1.796875, ((0, 4), (2, 32)))
    dinv = noise(streams_of[2], (S, POLES, SN, 2, S), 1.0, 6.0, ((0, 32), (1, 4)), jnp.float32)
    ancestors = draw_ancestors(jax.random.fold_in(streams_of[7], 71), 0)
    owner_keys = jax.random.split(jax.random.fold_in(streams_of[4], 1), NBLOCKS // HB)
    owner_turns = jax.random.permutation(jax.random.fold_in(streams_of[4], 3), NBLOCKS // HB)
    owner = jax.vmap(lambda own, number: routed_block(jax.random.fold_in(streams_of[4], 2), own, number, HB, TILES, 1, CAP, 2))(owner_keys, owner_turns).reshape((NBLOCKS, 1))
    weight_table = noise(streams_of[5], (2, NWEIGHT), 1.0, 4.0, (), jnp.float32)
    pole_slot = set_ends(jax.random.randint(streams_of[6], (POLES,), 0, NWEIGHT), jax.random.fold_in(streams_of[6], 1), 0, NWEIGHT - 1).astype(jnp.int32)
    return dict(inverse=inverse, factor=factor, dinv=dinv, ancestors=ancestors, owner=owner, weight_table=weight_table, pole_slot=pole_slot)


precise = lax.Precision.HIGHEST


def transposed(left, right):
    return lax.dot_general(left, right, (((0,), (0,)), ((), ())), preferred_element_type=jnp.float32)


def reference(inverse, factor, dinv, ancestors, owner, weight_table, pole_slot):
    count_blocks = A // BS
    choose_map = (jnp.arange(NWEIGHT)[None, :] == pole_slot[:, None]).astype(jnp.float32)
    weights = jnp.dot(choose_map, weight_table.T, precision=precise)
    block_of_row = jnp.arange(A) // BS
    selected = jnp.any(block_of_row[None, :, None] == ancestors[:, None, :], axis=2)
    columns = []
    diags = []
    for member in range(POLES):
        real_full = inverse[member, 0].reshape(A, count_blocks, BS)
        imag_full = inverse[member, 1].reshape(A, count_blocks, BS)
        col_list = []
        diag_list = []
        for supernode in range(SN):
            picked = ancestors[supernode]
            real_sel = jnp.take(real_full, picked, axis=1).reshape(A, NSEL * BS)
            imag_sel = jnp.take(imag_full, picked, axis=1).reshape(A, NSEL * BS)
            left_real = factor[member, supernode, :, :S]
            left_imag = factor[member, supernode, :, S:]
            prod_real = jnp.dot(real_sel, left_real, preferred_element_type=jnp.float32) - jnp.dot(imag_sel, left_imag, preferred_element_type=jnp.float32)
            prod_imag = jnp.dot(real_sel, left_imag, preferred_element_type=jnp.float32) + jnp.dot(imag_sel, left_real, preferred_element_type=jnp.float32)
            keep = selected[supernode][:, None]
            col_list.append(jnp.stack([jnp.where(keep, -prod_real, 0.0), jnp.where(keep, -prod_imag, 0.0)], axis=1))
            round_real = prod_real.astype(jnp.bfloat16).reshape(count_blocks, BS, S)
            round_imag = prod_imag.astype(jnp.bfloat16).reshape(count_blocks, BS, S)
            rows_real = jnp.take(round_real, picked, axis=0).reshape(NSEL * BS, S)
            rows_imag = jnp.take(round_imag, picked, axis=0).reshape(NSEL * BS, S)
            mat_real = transposed(left_real, rows_real) - transposed(left_imag, rows_imag)
            mat_imag = transposed(left_real, rows_imag) + transposed(left_imag, rows_real)
            diag_list.append(dinv[:, member, supernode] + jnp.stack([mat_real, mat_imag], axis=1))
        columns.append(jnp.stack(col_list, axis=1))
        diags.append(jnp.stack(diag_list, axis=1))
    inverse_column = jnp.stack(columns, axis=1)
    diag_inverse = jnp.stack(diags, axis=1)
    weight_real = weights[:, 0][None, :, None, None]
    weight_imag = weights[:, 1][None, :, None, None]
    density_diag = jnp.sum(weight_real * diag_inverse[:, :, :, 1] + weight_imag * diag_inverse[:, :, :, 0], axis=1)
    column_density = jnp.sum(weight_real * inverse_column[:, :, :, 1] + weight_imag * inverse_column[:, :, :, 0], axis=1)
    pieces = column_density.reshape(A // BR, BR, SN, S // BC, BC).transpose(0, 2, 3, 1, 4).reshape(NBLOCKS, BR * BC)
    tile_map = (jnp.arange(TILES)[:, None] == owner[None, :, 0]).astype(jnp.float32)
    tile_density = jnp.dot(tile_map, pieces, precision=precise).reshape(TILES, BR, BC)
    return inverse_column, diag_inverse, density_diag, tile_density
```

```python
import jax
import jax.numpy as jnp
from jax import lax
from jax.experimental import pallas as pl
from jax.experimental.pallas import tpu as pltpu
from jax.sharding import PartitionSpec as P

S = 512
BS = 128
NSEL = 16
NWEIGHT = 16
ROWS = 4
COLS = 8
POLES = 4
GRID = ROWS * COLS
LROWS = NSEL * BS // GRID
HALF = LROWS // 2
MESH = pl.DeviceIdType.MESH
BF = jnp.bfloat16
F32 = jnp.float32


def kernel(
    inverse,
    factor,
    dinv,
    ancestors,
    owner,
    table,
    slot,
    column_out,
    diag_out,
    density_out,
    tile_out,
    lbuf,
    gbuf,
    abuf,
    acc,
    col_buf,
    ysend,
    yrecv,
    dsend,
    drecv,
    pick,
    tsend,
    trecv,
    psend,
    precv,
    qsend,
    qrecv,
    local_sem,
    l_send,
    l_recv,
    h_send,
    h_recv,
    g_send,
    g_recv,
    y_send,
    y_recv,
    d_send,
    d_recv,
    t_send,
    t_recv,
    p_send,
    p_recv,
    q_send,
    q_recv,
    out_sem,
):
    pole, row, col = lax.axis_index("pole"), lax.axis_index("row"), lax.axis_index("col")
    side, depth = col // 4, col % 4
    me = row * COLS + col

    def plane(ds, dz):
        return ((side + ds) % 2) * 4 + (depth + dz) % 4

    def up(k):
        return (row + k) % ROWS

    def remote(src, dst, send, recv, to):
        return pltpu.make_async_remote_copy(
            src_ref=src,
            dst_ref=dst,
            send_sem=send,
            recv_sem=recv,
            device_id=to,
            device_id_type=MESH,
        )

    sends = []

    def go(copy):
        copy.start()
        sends.append(copy)

    own_factor = pltpu.make_async_copy(
        factor, lbuf.at[me // 2, pl.ds((me % 2) * LROWS, LROWS)], local_sem.at[0]
    )
    own_factor.start()

    def piece(c, k):
        return inverse.at[:, pl.ds(c * BS, BS), pl.ds(k * BS, BS)]

    for k in range(4):
        pltpu.make_async_copy(piece(col, k), gbuf.at[col * 4 + k], local_sem.at[1]).start()

    barrier = pltpu.get_barrier_semaphore()
    others = [(ds, dz) for ds in (0, 1) for dz in (0, 1, 3, 2) if (ds, dz) != (0, 0)]
    for ds, dz in others:
        pl.semaphore_signal(
            barrier, inc=1, device_id=(pole, row, plane(ds, dz)), device_id_type=MESH
        )
    for k in (1, 3, 2):
        pl.semaphore_signal(barrier, inc=1, device_id=(pole, up(k), col), device_id_type=MESH)
    for k in range(1, POLES):
        pl.semaphore_signal(
            barrier, inc=1, device_id=((pole + k) % POLES, row, col), device_id_type=MESH
        )
    pl.semaphore_wait(barrier, len(others) + ROWS - 1 + POLES - 1)
    own_factor.wait()

    def block(r, c):
        return lbuf.at[r * 4 + c // 2, pl.ds((c % 2) * LROWS, LROWS)]

    def half(r, c, part):
        return lbuf.at[r * 4 + c // 2, pl.ds((c % 2) * LROWS + part * HALF, HALF)]

    count = [0]

    def send_block(r, c, to):
        k = count[0]
        count[0] += 1
        go(remote(block(r, c), block(r, c), l_send.at[k], l_recv.at[r * COLS + c], to))

    def wait_block(r, c):
        remote(
            block(r, c), block(r, c), l_send.at[0], l_recv.at[r * COLS + c], (pole, row, col)
        ).wait_recv()

    halves = [0]

    def send_half(r, c, part, to):
        k = halves[0]
        halves[0] += 1
        go(
            remote(
                half(r, c, part), half(r, c, part), h_send.at[k], h_recv.at[part, c], to
            )
        )

    def wait_half(r, c, part):
        remote(
            half(r, c, part), half(r, c, part), h_send.at[0], h_recv.at[part, c], (pole, row, col)
        ).wait_recv()

    def along_rows(c):
        send_block(row, c, (pole, up(1), col))
        send_block(row, c, (pole, up(3), col))

    def pass_on(c):
        wait_block(up(3), c)
        send_half(up(3), c, 0, (pole, up(1), col))
        wait_block(up(1), c)
        send_half(up(1), c, 1, (pole, up(3), col))

    send_block(row, col, (pole, row, plane(1, 0)))
    along_rows(col)
    for dz in (1, 3, 2):
        send_block(row, col, (pole, row, plane(0, dz)))
    facing = plane(1, 0)
    wait_block(row, facing)
    along_rows(facing)
    for dz in (1, 3, 2):
        send_block(row, facing, (pole, row, plane(0, dz)))

    for n, (ds, dz) in enumerate(((1, 2), (1, 1), (1, 3), (1, 0), (0, 2), (0, 1), (0, 3))):
        c = plane(ds, dz)
        for k in range(4):
            remote(
                piece(c, k), gbuf.at[col * 4 + k], g_send.at[n], g_recv.at[col], (pole, row, c)
            ).start()

    def strip(c, n):
        four = gbuf.at[pl.ds(c * 4, 4)]
        return remote(four, four, g_send.at[n], g_recv.at[c], (pole, row, col))

    order = [plane(0, 0), plane(1, 0), plane(0, 1), plane(0, 3)]
    order += [plane(1, 1), plane(1, 3), plane(0, 2), plane(1, 2)]
    for k in (2, 3):
        wait_block(row, order[k])
        along_rows(order[k])
    pass_on(order[0])
    pass_on(order[1])
    for k in (4, 5):
        wait_block(row, order[k])
        along_rows(order[k])
    pass_on(order[2])
    for k in (6, 7):
        wait_block(row, order[k])
        along_rows(order[k])
    for k in range(3, 8):
        pass_on(order[k])

    lane = lax.broadcasted_iota(jnp.int32, (64, 512), 1)
    owner_index = lax.broadcasted_iota(jnp.int32, (64, 512), 0)
    mine = ((lane & 127) >> 3) * 4 + (lane >> 7)
    target = owner[...]
    target = ((target & 31) * 32 + (target >> 5) * 8).astype(F32)
    spread = jnp.where(mine == owner_index, target, 0.0)
    key = jnp.sum(spread, axis=0, keepdims=True) + (lane[:1] & 7).astype(F32)
    position = lax.broadcasted_iota(jnp.int32, (1024, 512), 0).astype(F32)
    pick[...] = jnp.where(position == key, 1.0, 0.0).astype(BF)

    mine = gbuf.at[pl.ds(col * 4, 4)]
    pltpu.make_async_copy(mine, mine, local_sem.at[1]).wait()
    for ds, dz in others:
        strip(plane(ds, dz), 0).wait_recv()
    for i in range(NSEL):
        for part in range(2):
            abuf[i // 4, part * BS : (part + 1) * BS, (i % 4) * BS : (i % 4 + 1) * BS] = gbuf[
                ancestors[0, i], part
            ]

    def product(r):
        right = lbuf[pl.ds(r * 4, 4)].reshape(4 * BS, 2 * S)
        return jnp.dot(abuf[r], right, preferred_element_type=F32)

    acc[...] = product(row)
    acc[...] += product(up(1))
    acc[...] += product(up(3))
    for c in order:
        wait_half(up(2), c, 0)
        wait_half(up(2), c, 1)
    acc[...] += product(up(2))

    real = acc[:BS, :S] - acc[BS:, S:]
    imag = acc[:BS, S:] + acc[BS:, :S]

    chosen = jnp.int32(0)
    for i in range(NSEL):
        chosen += jnp.where(ancestors[0, i] == me, 1, 0)
    keep = lax.broadcast_in_dim(chosen, (BS, S), ()) > 0
    real = jnp.where(keep, real, 0.0)
    imag = jnp.where(keep, imag, 0.0)
    col_buf[0] = -real
    col_buf[1] = -imag
    column_copy = pltpu.make_async_copy(col_buf, column_out, out_sem)
    column_copy.start()
    for q in range(4):
        lanes = slice(q * BS, (q + 1) * BS)
        ysend[q] = jnp.concatenate([real[:, lanes], imag[:, lanes]], axis=1).astype(BF)
    for k in (2, 1, 3):
        r = up(k)
        go(remote(ysend.at[r], yrecv.at[row], y_send.at[k], y_recv.at[row], (pole, r, col)))
    yrecv[row] = ysend[row]

    weight_real = table[0, slot[0]]
    weight_imag = table[1, slot[0]]
    share = -(weight_real * imag + weight_imag * real)
    share = jnp.concatenate([share[:, q * BS : (q + 1) * BS] for q in range(4)], axis=0)
    high = share.astype(BF)
    low = (share - high.astype(F32)).astype(BF)
    tiles = jnp.dot(pick[...], jnp.concatenate([high, low], axis=1), preferred_element_type=F32)
    tiles = tiles[:, :BS] + tiles[:, BS:]
    tsend[...] = tiles.astype(BF).reshape(GRID, 32, BS)

    def to_position(k):
        to = (me + k) % GRID
        return to, (pole, to // COLS, to % COLS)

    def send_tiles(k, carry):
        to, device = to_position(k)
        remote(tsend.at[to], trecv.at[me], t_send, t_recv, device).start()
        return carry

    lax.fori_loop(1, GRID, send_tiles, 0)
    trecv[me] = tsend[me]

    for k in (1, 3, 2):
        r = up(k)
        remote(ysend.at[0], yrecv.at[r], y_send.at[0], y_recv.at[r], (pole, row, col)).wait_recv()
    lefts = []
    for r in range(4):
        b = r * COLS + col
        before = jnp.int32(0)
        for i in range(NSEL):
            before += jnp.where(ancestors[0, i] < b, 1, 0)
        before = jnp.minimum(before, NSEL - 1)
        lefts.append(lbuf[before])
    left = jnp.concatenate(lefts, axis=0)
    mixed = lax.dot_general(
        left, yrecv[...].reshape(4 * BS, 2 * BS), (((0,), (0,)), ((), ())), preferred_element_type=F32
    )
    diag_real = mixed[:S, :BS] - mixed[S:, BS:]
    diag_imag = mixed[:S, BS:] + mixed[S:, :BS]
    dsend[...] = (
        jnp.concatenate([diag_real, diag_imag], axis=1).astype(BF).reshape(GRID, S // GRID, 2 * BS)
    )

    def send_diag(k, carry):
        to, device = to_position(k)
        remote(dsend.at[to], drecv.at[me], d_send, d_recv, device).start()
        return carry

    lax.fori_loop(1, GRID, send_diag, 0)
    drecv[me] = dsend[me]

    most = pl.ds(0, GRID - 1)
    arrived = remote(tsend.at[most], trecv.at[most], t_send, t_recv, (pole, row, col))
    arrived.wait_recv()
    total = jnp.sum(trecv[...].astype(F32), axis=0)
    psend[...] = total.reshape(POLES, 8, BS)
    for k in range(1, POLES):
        p = (pole + k) % POLES
        go(remote(psend.at[p], precv.at[pole], p_send.at[k], p_recv.at[pole], (p, row, col)))
    precv[pole] = psend[pole]

    landed = remote(dsend.at[most], drecv.at[most], d_send, d_recv, (pole, row, col))
    landed.wait_recv()
    dreal, dimag = [], []
    for q in range(4):
        quarter = jnp.sum(drecv[q * COLS : (q + 1) * COLS].astype(F32), axis=0)
        dreal.append(quarter[:, :BS])
        dimag.append(quarter[:, BS:])
    dreal = jnp.concatenate(dreal, axis=1) + dinv[:, 0, :]
    dimag = jnp.concatenate(dimag, axis=1) + dinv[:, 1, :]
    diag_out[:, 0, :] = dreal
    diag_out[:, 1, :] = dimag
    qsend[...] = weight_real * dimag + weight_imag * dreal
    for k in range(1, POLES):
        p = (pole + k) % POLES
        go(remote(qsend, qrecv.at[pole], q_send.at[k], q_recv.at[pole], (p, row, col)))
    qrecv[pole] = qsend[...]
    for k in range(1, POLES):
        p = (pole + k) % POLES
        remote(psend.at[0], precv.at[p], p_send.at[0], p_recv.at[p], (pole, row, col)).wait_recv()
    tile_out[...] = jnp.sum(precv[...], axis=0)
    for k in range(1, POLES):
        p = (pole + k) % POLES
        remote(qsend, qrecv.at[p], q_send.at[0], q_recv.at[p], (pole, row, col)).wait_recv()
    density_out[...] = jnp.sum(qrecv[...], axis=0)

    arrived.wait_send()
    landed.wait_send()
    for copy in sends:
        copy.wait_send()
    for n in range(COLS - 1):
        strip(col, n).wait_send()
    column_copy.wait()


def body(inverse, factor, dinv, ancestors, owner, weight_table, pole_slot):
    vmem = pl.BlockSpec(memory_space=pltpu.VMEM)
    smem = pl.BlockSpec(memory_space=pltpu.SMEM)
    hbm = pl.BlockSpec(memory_space=pl.ANY)
    dma = pltpu.SemaphoreType.DMA
    column, diag, density, tile = pl.pallas_call(
        kernel,
        name="supernode",
        out_shape=(
            jax.ShapeDtypeStruct((2, BS, S), F32),
            jax.ShapeDtypeStruct((S // GRID, 2, S), F32),
            jax.ShapeDtypeStruct((S // GRID, S), F32),
            jax.ShapeDtypeStruct((8, BS), F32),
        ),
        in_specs=[hbm, hbm, vmem, smem, vmem, smem, smem],
        out_specs=(hbm, vmem, vmem, vmem),
        scratch_shapes=[
            pltpu.VMEM((NSEL, BS, 2 * S), BF),
            pltpu.VMEM((COLS * 4, 2, BS, BS), BF),
            pltpu.VMEM((4, 2 * BS, 4 * BS), BF),
            pltpu.VMEM((2 * BS, 2 * S), F32),
            pltpu.VMEM((2, BS, S), F32),
            pltpu.VMEM((4, BS, 2 * BS), BF),
            pltpu.VMEM((4, BS, 2 * BS), BF),
            pltpu.VMEM((GRID, S // GRID, 2 * BS), BF),
            pltpu.VMEM((GRID, S // GRID, 2 * BS), BF),
            pltpu.VMEM((1024, 512), BF),
            pltpu.VMEM((GRID, 32, BS), BF),
            pltpu.VMEM((GRID, 32, BS), BF),
            pltpu.VMEM((POLES, 8, BS), F32),
            pltpu.VMEM((POLES, 8, BS), F32),
            pltpu.VMEM((S // GRID, S), F32),
            pltpu.VMEM((POLES, S // GRID, S), F32),
            dma((2,)),
            dma((24,)),
            dma((GRID,)),
            dma((16,)),
            dma((2, COLS)),
            dma((7,)),
            dma((COLS,)),
            dma((4,)),
            dma((4,)),
            dma,
            dma,
            dma,
            dma,
            dma((POLES,)),
            dma((POLES,)),
            dma((POLES,)),
            dma((POLES,)),
            dma,
        ],
        compiler_params=pltpu.CompilerParams(
            collective_id=0, has_side_effects=True, vmem_limit_bytes=48 << 20
        ),
    )(
        inverse.reshape(2, 1024, 512),
        factor.reshape(LROWS, 2 * S),
        dinv.reshape(S // GRID, 2, S),
        ancestors,
        owner,
        weight_table,
        pole_slot,
    )
    column = column.transpose(1, 0, 2).reshape(BS, 1, 1, 2, S)
    return (
        column,
        diag.reshape(S // GRID, 1, 1, 2, S),
        density.reshape(S // GRID, 1, S),
        tile.reshape(1, 8, BS),
    )


def solution(mesh):
    grid = ("row", "col")
    in_specs = (
        P("pole", None, "row", "col"),
        P("pole", None, grid, None),
        P(grid, "pole", None, None, None),
        P(),
        P(grid, None),
        P(),
        P("pole"),
    )
    out_specs = (
        P(grid, "pole", None, None, None),
        P(grid, "pole", None, None, None),
        P(grid, None, None),
        P(("pole", "row", "col"), None, None),
    )
    return jax.shard_map(body, mesh=mesh, in_specs=in_specs, out_specs=out_specs, check_vma=False)
```

```python
import jax
import jax.numpy as jnp
from jax import lax
from jax.experimental import pallas as pl
from jax.experimental.pallas import tpu as pltpu
from jax.sharding import PartitionSpec as P

S = 512
BS = 128
NSEL = 16
NWEIGHT = 16
ROWS = 4
COLS = 8
POLES = 4
GRID = ROWS * COLS
LROWS = NSEL * BS // GRID
HALF = LROWS // 2
MESH = pl.DeviceIdType.MESH
BF = jnp.bfloat16
F32 = jnp.float32


def kernel(
    inverse,
    factor,
    dinv_in,
    ancestors_in,
    owner_in,
    table_in,
    slot,
    column_out,
    diag_out,
    density_out,
    tile_out,
    lbuf,
    gbuf,
    abuf,
    acc,
    dinv,
    owner,
    ancestors,
    table,
    ysend,
    yrecv,
    dsend,
    drecv,
    pick,
    tsend,
    trecv,
    psend,
    precv,
    qsend,
    qrecv,
    local_sem,
    l_send,
    l_recv,
    h_send,
    h_recv,
    g_send,
    g_recv,
    y_send,
    y_recv,
    d_send,
    d_recv,
    t_send,
    t_recv,
    p_send,
    p_recv,
    q_send,
    q_recv,
):
    pole, row, col = lax.axis_index("pole"), lax.axis_index("row"), lax.axis_index("col")
    side, depth = col // 4, col % 4
    me = row * COLS + col

    def plane(ds, dz):
        return ((side + ds) % 2) * 4 + (depth + dz) % 4

    def up(k):
        return (row + k) % ROWS

    def remote(src, dst, send, recv, to):
        return pltpu.make_async_remote_copy(
            src_ref=src,
            dst_ref=dst,
            send_sem=send,
            recv_sem=recv,
            device_id=to,
            device_id_type=MESH,
        )

    sends = []

    def go(copy):
        copy.start()
        sends.append(copy)

    own_factor = pltpu.make_async_copy(
        factor, lbuf.at[me // 2, pl.ds((me % 2) * LROWS, LROWS)], local_sem.at[0]
    )
    own_factor.start()

    def piece(c, k):
        return inverse.at[:, pl.ds(c * BS, BS), pl.ds(k * BS, BS)]

    for k in range(4):
        pltpu.make_async_copy(piece(col, k), gbuf.at[col * 4 + k], local_sem.at[1]).start()

    small = [
        pltpu.make_async_copy(source, target, local_sem.at[2 + n])
        for n, (source, target) in enumerate(
            (
                (owner_in, owner),
                (ancestors_in, ancestors),
                (table_in, table),
                (dinv_in, dinv),
            )
        )
    ]
    for copy in small:
        copy.start()

    barrier = pltpu.get_barrier_semaphore()
    others = [(ds, dz) for ds in (0, 1) for dz in (0, 1, 3, 2) if (ds, dz) != (0, 0)]
    for ds, dz in others:
        pl.semaphore_signal(
            barrier, inc=1, device_id=(pole, row, plane(ds, dz)), device_id_type=MESH
        )
    for k in (1, 3, 2):
        pl.semaphore_signal(barrier, inc=1, device_id=(pole, up(k), col), device_id_type=MESH)
    for k in range(1, POLES):
        pl.semaphore_signal(
            barrier, inc=1, device_id=((pole + k) % POLES, row, col), device_id_type=MESH
        )
    pl.semaphore_wait(barrier, len(others) + ROWS - 1 + POLES - 1)
    own_factor.wait()

    def block(r, c):
        return lbuf.at[r * 4 + c // 2, pl.ds((c % 2) * LROWS, LROWS)]

    def half(r, c, part):
        return lbuf.at[r * 4 + c // 2, pl.ds((c % 2) * LROWS + part * HALF, HALF)]

    count = [0]

    def send_block(r, c, to):
        k = count[0]
        count[0] += 1
        go(remote(block(r, c), block(r, c), l_send.at[k], l_recv.at[r * COLS + c], to))

    def wait_block(r, c):
        remote(
            block(r, c), block(r, c), l_send.at[0], l_recv.at[r * COLS + c], (pole, row, col)
        ).wait_recv()

    halves = [0]

    def send_half(r, c, part, to):
        k = halves[0]
        halves[0] += 1
        go(
            remote(
                half(r, c, part), half(r, c, part), h_send.at[k], h_recv.at[part, c], to
            )
        )

    def wait_half(r, c, part):
        remote(
            half(r, c, part), half(r, c, part), h_send.at[0], h_recv.at[part, c], (pole, row, col)
        ).wait_recv()

    def along_rows(c):
        send_block(row, c, (pole, up(1), col))
        send_block(row, c, (pole, up(3), col))

    def pass_on(c):
        wait_block(up(3), c)
        send_half(up(3), c, 0, (pole, up(1), col))
        wait_block(up(1), c)
        send_half(up(1), c, 1, (pole, up(3), col))

    send_block(row, col, (pole, row, plane(1, 0)))
    along_rows(col)
    for dz in (1, 3, 2):
        send_block(row, col, (pole, row, plane(0, dz)))
    facing = plane(1, 0)
    wait_block(row, facing)
    along_rows(facing)
    for dz in (1, 3, 2):
        send_block(row, facing, (pole, row, plane(0, dz)))

    for n, (ds, dz) in enumerate(((1, 2), (1, 1), (1, 3), (1, 0), (0, 2), (0, 1), (0, 3))):
        c = plane(ds, dz)
        for k in range(4):
            remote(
                piece(c, k), gbuf.at[col * 4 + k], g_send.at[n], g_recv.at[col], (pole, row, c)
            ).start()

    def strip(c, n):
        four = gbuf.at[pl.ds(c * 4, 4)]
        return remote(four, four, g_send.at[n], g_recv.at[c], (pole, row, col))

    order = [plane(0, 0), plane(1, 0), plane(0, 1), plane(0, 3)]
    order += [plane(1, 1), plane(1, 3), plane(0, 2), plane(1, 2)]
    for k in (2, 3):
        wait_block(row, order[k])
        along_rows(order[k])
    pass_on(order[0])
    pass_on(order[1])
    for k in (4, 5):
        wait_block(row, order[k])
        along_rows(order[k])
    pass_on(order[2])
    for k in (6, 7):
        wait_block(row, order[k])
        along_rows(order[k])
    for k in range(3, 8):
        pass_on(order[k])

    lane = lax.broadcasted_iota(jnp.int32, (64, 512), 1)
    owner_index = lax.broadcasted_iota(jnp.int32, (64, 512), 0)
    mine = ((lane & 127) >> 3) * 4 + (lane >> 7)
    for copy in small:
        copy.wait()
    across = lax.broadcasted_iota(jnp.int32, (64, 64), 1)
    down = lax.broadcasted_iota(jnp.int32, (64, 64), 0)
    target = jnp.where(across == down, owner[...].astype(F32), 0.0)
    target = jnp.sum(target, axis=1, keepdims=True).astype(jnp.int32)
    target = ((target & 31) * 32 + (target >> 5) * 8).astype(F32)
    spread = jnp.where(mine == owner_index, target, 0.0)
    key = jnp.sum(spread, axis=0, keepdims=True) + (lane[:1] & 7).astype(F32)
    position = lax.broadcasted_iota(jnp.int32, (1024, 512), 0).astype(F32)
    pick[...] = jnp.where(position == key, 1.0, 0.0).astype(BF)

    mine = gbuf.at[pl.ds(col * 4, 4)]
    pltpu.make_async_copy(mine, mine, local_sem.at[1]).wait()
    for ds, dz in others:
        strip(plane(ds, dz), 0).wait_recv()
    for i in range(NSEL):
        for part in range(2):
            abuf[i // 4, part * BS : (part + 1) * BS, (i % 4) * BS : (i % 4 + 1) * BS] = gbuf[
                ancestors[0, i], part
            ]

    def product(r):
        right = lbuf[pl.ds(r * 4, 4)].reshape(4 * BS, 2 * S)
        return jnp.dot(abuf[r], right, preferred_element_type=F32)

    acc[...] = product(row)
    acc[...] += product(up(1))
    acc[...] += product(up(3))
    for c in order:
        wait_half(up(2), c, 0)
        wait_half(up(2), c, 1)
    acc[...] += product(up(2))

    real = acc[:BS, :S] - acc[BS:, S:]
    imag = acc[:BS, S:] + acc[BS:, :S]

    chosen = jnp.int32(0)
    for i in range(NSEL):
        chosen += jnp.where(ancestors[0, i] == me, 1, 0)
    keep = lax.broadcast_in_dim(chosen, (BS, S), ()) > 0
    real = jnp.where(keep, real, 0.0)
    imag = jnp.where(keep, imag, 0.0)
    for q in range(4):
        lanes = slice(q * BS, (q + 1) * BS)
        ysend[q] = jnp.concatenate([real[:, lanes], imag[:, lanes]], axis=1).astype(BF)
    for k in (2, 1, 3):
        r = up(k)
        go(remote(ysend.at[r], yrecv.at[row], y_send.at[k], y_recv.at[row], (pole, r, col)))
    yrecv[row] = ysend[row]

    weight_real = table[0, slot[0]]
    weight_imag = table[1, slot[0]]
    share = -(weight_real * imag + weight_imag * real)
    share = jnp.concatenate([share[:, q * BS : (q + 1) * BS] for q in range(4)], axis=0)
    high = share.astype(BF)
    low = (share - high.astype(F32)).astype(BF)
    tiles = jnp.dot(pick[...], jnp.concatenate([high, low], axis=1), preferred_element_type=F32)
    tiles = tiles[:, :BS] + tiles[:, BS:]
    tsend[...] = tiles.astype(BF).reshape(GRID, 32, BS)

    def to_position(k):
        to = (me + k) % GRID
        return to, (pole, to // COLS, to % COLS)

    def send_tiles(k, carry):
        to, device = to_position(k)
        remote(tsend.at[to], trecv.at[me], t_send, t_recv, device).start()
        return carry

    lax.fori_loop(1, GRID, send_tiles, 0)
    trecv[me] = tsend[me]
    column_out[:, 0, :] = -real
    column_out[:, 1, :] = -imag

    for k in (1, 3, 2):
        r = up(k)
        remote(ysend.at[0], yrecv.at[r], y_send.at[0], y_recv.at[r], (pole, row, col)).wait_recv()
    lefts = []
    for r in range(4):
        b = r * COLS + col
        before = jnp.int32(0)
        for i in range(NSEL):
            before += jnp.where(ancestors[0, i] < b, 1, 0)
        before = jnp.minimum(before, NSEL - 1)
        lefts.append(lbuf[before])
    left = jnp.concatenate(lefts, axis=0)
    mixed = lax.dot_general(
        left, yrecv[...].reshape(4 * BS, 2 * BS), (((0,), (0,)), ((), ())), preferred_element_type=F32
    )
    diag_real = mixed[:S, :BS] - mixed[S:, BS:]
    diag_imag = mixed[:S, BS:] + mixed[S:, :BS]
    dsend[...] = (
        jnp.concatenate([diag_real, diag_imag], axis=1).astype(BF).reshape(GRID, S // GRID, 2 * BS)
    )

    def send_diag(k, carry):
        to, device = to_position(k)
        remote(dsend.at[to], drecv.at[me], d_send, d_recv, device).start()
        return carry

    lax.fori_loop(1, GRID, send_diag, 0)
    drecv[me] = dsend[me]

    most = pl.ds(0, GRID - 1)
    arrived = remote(tsend.at[most], trecv.at[most], t_send, t_recv, (pole, row, col))
    arrived.wait_recv()
    total = jnp.sum(trecv[...].astype(F32), axis=0)
    psend[...] = total.reshape(POLES, 8, BS)
    for k in range(1, POLES):
        p = (pole + k) % POLES
        go(remote(psend.at[p], precv.at[pole], p_send.at[k], p_recv.at[pole], (p, row, col)))
    precv[pole] = psend[pole]

    landed = remote(dsend.at[most], drecv.at[most], d_send, d_recv, (pole, row, col))
    landed.wait_recv()
    dreal, dimag = [], []
    for q in range(4):
        quarter = jnp.sum(drecv[q * COLS : (q + 1) * COLS].astype(F32), axis=0)
        dreal.append(quarter[:, :BS])
        dimag.append(quarter[:, BS:])
    dreal = jnp.concatenate(dreal, axis=1) + dinv[:, 0, :]
    dimag = jnp.concatenate(dimag, axis=1) + dinv[:, 1, :]
    diag_out[:, 0, :] = dreal
    diag_out[:, 1, :] = dimag
    qsend[...] = weight_real * dimag + weight_imag * dreal
    for k in range(1, POLES):
        p = (pole + k) % POLES
        go(remote(qsend, qrecv.at[pole], q_send.at[k], q_recv.at[pole], (p, row, col)))
    qrecv[pole] = qsend[...]
    for k in range(1, POLES):
        p = (pole + k) % POLES
        remote(psend.at[0], precv.at[p], p_send.at[0], p_recv.at[p], (pole, row, col)).wait_recv()
    tile_out[...] = jnp.sum(precv[...], axis=0)
    for k in range(1, POLES):
        p = (pole + k) % POLES
        remote(qsend, qrecv.at[p], q_send.at[0], q_recv.at[p], (pole, row, col)).wait_recv()
    density_out[:, 0, :] = jnp.sum(qrecv[...], axis=0)

    arrived.wait_send()
    landed.wait_send()
    for copy in sends:
        copy.wait_send()
    for n in range(COLS - 1):
        strip(col, n).wait_send()


def hand_out(*refs):
    done = refs[8]
    copies = [pltpu.make_async_copy(refs[k], refs[4 + k], done.at[k]) for k in range(4)]
    for copy in copies:
        copy.start()
    for copy in copies:
        copy.wait()


def body(inverse, factor, dinv, ancestors, owner, weight_table, pole_slot):
    vmem = pl.BlockSpec(memory_space=pltpu.VMEM)
    hbm = pl.BlockSpec(memory_space=pl.ANY)
    dma = pltpu.SemaphoreType.DMA
    column, diag, density, tile = pl.pallas_call(
        kernel,
        name="supernode",
        out_shape=(
            pltpu.VMEM((BS, 2, S), F32),
            pltpu.VMEM((S // GRID, 2, S), F32),
            pltpu.VMEM((S // GRID, 1, S), F32),
            pltpu.VMEM((8, BS), F32),
        ),
        in_specs=[pl.BlockSpec(memory_space=pltpu.HBM)] * 6 + [pl.BlockSpec(memory_space=pltpu.SMEM)],
        out_specs=(vmem,) * 4,
        scratch_shapes=[
            pltpu.VMEM((NSEL, BS, 2 * S), BF),
            pltpu.VMEM((COLS * 4, 2, BS, BS), BF),
            pltpu.VMEM((4, 2 * BS, 4 * BS), BF),
            pltpu.VMEM((2 * BS, 2 * S), F32),
            pltpu.VMEM((S // GRID, 2, S), F32),
            pltpu.VMEM((1, 64), jnp.int32),
            pltpu.SMEM((1, NSEL), jnp.int32),
            pltpu.SMEM((2, NWEIGHT), F32),
            pltpu.VMEM((4, BS, 2 * BS), BF),
            pltpu.VMEM((4, BS, 2 * BS), BF),
            pltpu.VMEM((GRID, S // GRID, 2 * BS), BF),
            pltpu.VMEM((GRID, S // GRID, 2 * BS), BF),
            pltpu.VMEM((1024, 512), BF),
            pltpu.VMEM((GRID, 32, BS), BF),
            pltpu.VMEM((GRID, 32, BS), BF),
            pltpu.VMEM((POLES, 8, BS), F32),
            pltpu.VMEM((POLES, 8, BS), F32),
            pltpu.VMEM((S // GRID, S), F32),
            pltpu.VMEM((POLES, S // GRID, S), F32),
            dma((7,)),
            dma((24,)),
            dma((GRID,)),
            dma((16,)),
            dma((2, COLS)),
            dma((7,)),
            dma((COLS,)),
            dma((4,)),
            dma((4,)),
            dma,
            dma,
            dma,
            dma,
            dma((POLES,)),
            dma((POLES,)),
            dma((POLES,)),
            dma((POLES,)),
        ],
        compiler_params=pltpu.CompilerParams(
            collective_id=0, has_side_effects=True, vmem_limit_bytes=56 << 20
        ),
    )(
        *(
            pltpu.with_memory_space_constraint(x, pltpu.HBM)
            for x in (
                inverse.reshape(2, 1024, 512),
                factor.reshape(LROWS, 2 * S),
                dinv.reshape(S // GRID, 2, S),
                ancestors,
                owner.reshape(1, 64),
                weight_table,
            )
        ),
        pole_slot,
    )
    column, diag, density, tile = pl.pallas_call(
        hand_out,
        name="hand_out",
        out_shape=tuple(jax.ShapeDtypeStruct(x.shape, F32) for x in (column, diag, density, tile)),
        in_specs=[vmem] * 4,
        out_specs=(hbm,) * 4,
        scratch_shapes=[dma((4,))],
        compiler_params=pltpu.CompilerParams(vmem_limit_bytes=1 << 20),
    )(column, diag, density, tile)
    return (
        column.reshape(BS, 1, 1, 2, S),
        diag.reshape(S // GRID, 1, 1, 2, S),
        density,
        tile.reshape(1, 8, BS),
    )


def solution(mesh):
    grid = ("row", "col")
    in_specs = (
        P("pole", None, "row", "col"),
        P("pole", None, grid, None),
        P(grid, "pole", None, None, None),
        P(),
        P(grid, None),
        P(),
        P("pole"),
    )
    out_specs = (
        P(grid, "pole", None, None, None),
        P(grid, "pole", None, None, None),
        P(grid, None, None),
        P(("pole", "row", "col"), None, None),
    )
    return jax.shard_map(body, mesh=mesh, in_specs=in_specs, out_specs=out_specs, check_vma=False)
```

```python
import jax
import jax.numpy as jnp
from jax import lax
from jax.experimental import pallas as pl
from jax.experimental.pallas import tpu as pltpu
from jax.sharding import PartitionSpec as P

S = 512
BS = 128
NSEL = 16
NWEIGHT = 16
ROWS = 4
COLS = 8
POLES = 4
GRID = ROWS * COLS
LROWS = NSEL * BS // GRID
HALF = LROWS // 2
MESH = pl.DeviceIdType.MESH
BF = jnp.bfloat16
F32 = jnp.float32


def kernel(
    inverse,
    factor,
    dinv_in,
    ancestors_in,
    owner_in,
    table_in,
    slot,
    column_out,
    diag_out,
    density_out,
    tile_out,
    lbuf,
    first_strips,
    second_strips,
    abuf,
    left,
    column_send,
    dinv,
    owner,
    ancestors,
    table,
    ysend,
    yrecv,
    dsend,
    drecv,
    pick,
    tsend,
    trecv,
    psend,
    precv,
    qsend,
    qrecv,
    local_sem,
    l_send,
    l_recv,
    h_send,
    h_recv,
    g_send,
    g_recv,
    o_send,
    o_recv,
    c_send,
    c_recv,
    y_send,
    y_recv,
    d_send,
    d_recv,
    t_send,
    t_recv,
    p_send,
    p_recv,
    q_send,
    q_recv,
):
    pole, row, col = lax.axis_index("pole"), lax.axis_index("row"), lax.axis_index("col")
    side, depth = col // 4, col % 4
    me = row * COLS + col
    works = pole % 2
    active = side == works
    facing = (1 - side) * 4 + depth
    source = row * 4 + depth
    turns = (1 - works, works)
    strips = (first_strips, second_strips)

    def at_depth(s, dz):
        return s * 4 + (depth + dz) % 4

    def up(k):
        return (row + k) % ROWS

    def remote(src, dst, send, recv, to):
        return pltpu.make_async_remote_copy(
            src_ref=src,
            dst_ref=dst,
            send_sem=send,
            recv_sem=recv,
            device_id=to,
            device_id_type=MESH,
        )

    here = (pole, row, col)

    def sent(ref, send):
        remote(ref, ref, send, q_recv.at[0], here).wait_send()

    def came(ref, recv):
        remote(ref, ref, q_send.at[0], recv, here).wait_recv()

    own_factor = pltpu.make_async_copy(
        factor, lbuf.at[me // 2, pl.ds((me % 2) * LROWS, LROWS)], local_sem.at[0]
    )
    own_factor.start()
    small = [
        pltpu.make_async_copy(source, target, local_sem.at[2 + n])
        for n, (source, target) in enumerate(
            (
                (owner_in, owner.at[side]),
                (ancestors_in, ancestors),
                (table_in, table),
                (dinv_in, dinv),
            )
        )
    ]
    for copy in small:
        copy.start()

    def piece(rb, z, k):
        return inverse.at[:, pl.ds((rb * 4 + z) * BS, BS), pl.ds(k * BS, BS)]

    @pl.when(active)
    def _():
        for j, rb in enumerate(turns):
            for k in range(4):
                pltpu.make_async_copy(
                    piece(rb, depth, k), strips[j].at[col * 4 + k], local_sem.at[6 * j + 1]
                ).start()

    barrier = pltpu.get_barrier_semaphore()
    others = [(ds, dz) for ds in (0, 1) for dz in (0, 1, 3, 2) if (ds, dz) != (0, 0)]
    for ds, dz in others:
        c = ((side + ds) % 2) * 4 + (depth + dz) % 4
        pl.semaphore_signal(barrier, inc=1, device_id=(pole, row, c), device_id_type=MESH)
    for k in (1, 3, 2):
        pl.semaphore_signal(barrier, inc=1, device_id=(pole, up(k), col), device_id_type=MESH)
    for k in range(1, POLES):
        pl.semaphore_signal(
            barrier, inc=1, device_id=((pole + k) % POLES, row, col), device_id_type=MESH
        )
    pl.semaphore_wait(barrier, len(others) + ROWS - 1 + POLES - 1)
    own_factor.wait()
    for copy in small:
        copy.wait()

    def block(r, c):
        return lbuf.at[r * 4 + c // 2, pl.ds((c % 2) * LROWS, LROWS)]

    def half(r, c, part):
        return lbuf.at[r * 4 + c // 2, pl.ds((c % 2) * LROWS + part * HALF, HALF)]

    def send_strip(n, j, z):
        for k in range(4):
            remote(
                piece(turns[j], z, k),
                strips[j].at[col * 4 + k],
                g_send.at[n],
                g_recv.at[j, col],
                (pole, row, works * 4 + z),
            ).start()

    @pl.when(jnp.logical_not(active))
    def _():
        remote(
            block(row, col), block(row, col), l_send.at[0], l_recv.at[me], (pole, row, facing)
        ).start()
        remote(owner.at[side], owner.at[side], o_send, o_recv, (pole, row, facing)).start()
        n = 0
        for j in range(2):
            for dz in (2, 1, 3, 0):
                send_strip(n, j, (depth + dz) % 4)
                n += 1

    weight_real = table[0, slot[0]]
    weight_imag = table[1, slot[0]]

    def to_position(k):
        to = (me + k) % GRID
        return to, (pole, to // COLS, to % COLS)

    @pl.when(active)
    def _():
        count = [0]

        def send_block(r, c, to):
            k = count[0]
            count[0] += 1
            remote(
                block(r, c), block(r, c), l_send.at[k], l_recv.at[r * COLS + c], to
            ).start()

        def send_half(r, c, part, k, to):
            remote(
                half(r, c, part), half(r, c, part), h_send.at[k], h_recv.at[part, c], to
            ).start()

        def wait_block(r, c):
            came(block(r, c), l_recv.at[r * COLS + c])

        def along_rows(c):
            send_block(row, c, (pole, up(1), col))
            send_block(row, c, (pole, up(3), col))

        for c in (col, facing):
            if c is facing:
                wait_block(row, facing)
            for dz in (1, 3, 2):
                send_block(row, c, (pole, row, at_depth(side, dz)))
            along_rows(c)
        n = 0
        for j in range(2):
            for dz in (2, 1, 3):
                send_strip(n, j, (depth + dz) % 4)
                n += 1
        order = [col, facing]
        for dz in (1, 3, 2):
            order += [at_depth(side, dz), at_depth(1 - side, dz)]
        for c in order[2:]:
            wait_block(row, c)
            along_rows(c)
        for k, c in enumerate(order):
            wait_block(up(3), c)
            send_half(up(3), c, 0, 2 * k, (pole, up(1), col))
            wait_block(up(1), c)
            send_half(up(1), c, 1, 2 * k + 1, (pole, up(3), col))

        came(owner.at[0], o_recv)
        lane = lax.broadcasted_iota(jnp.int32, (64, 512), 1)
        owner_index = lax.broadcasted_iota(jnp.int32, (64, 512), 0)
        named = ((lane & 127) >> 3) * 4 + (lane >> 7)
        across = lax.broadcasted_iota(jnp.int32, (64, 64), 1)
        down = lax.broadcasted_iota(jnp.int32, (64, 64), 0)
        position = lax.broadcasted_iota(jnp.int32, (1024, 512), 0).astype(F32)
        for s in range(2):
            target = jnp.where(across == down, owner[s].astype(F32), 0.0)
            target = jnp.sum(target, axis=1, keepdims=True).astype(jnp.int32)
            target = ((target & 31) * 32 + (target >> 5) * 8).astype(F32)
            spread = jnp.where(named == owner_index, target, 0.0)
            key = jnp.sum(spread, axis=0, keepdims=True) + (lane[:1] & 7).astype(F32)
            pick[:, s * 512 : (s + 1) * 512] = jnp.where(position == key, 1.0, 0.0).astype(BF)

        for c in order:
            came(half(up(2), c, 0), h_recv.at[0, c])
            came(half(up(2), c, 1), h_recv.at[1, c])
        for r in range(4):
            for s in range(2):
                b = r * COLS + s * 4 + depth
                before = jnp.int32(0)
                for i in range(NSEL):
                    before += jnp.where(ancestors[0, i] < b, 1, 0)
                before = jnp.minimum(before, NSEL - 1)
                at = (2 * r + s) * BS
                left[:, at : at + BS] = lbuf[before].T

        shares = [None, None]
        columns = []
        for j, rb in enumerate(turns):
            for s in (0, 1):
                for dz in (1, 3, 2, 0):
                    c = at_depth(s, dz)

                    @pl.when(c != col)
                    def _():
                        came(strips[j].at[pl.ds(0, 4)], g_recv.at[j, c])

            own = strips[j].at[pl.ds(col * 4, 4)]
            pltpu.make_async_copy(own, own, local_sem.at[6 * j + 1]).wait()
            for i in range(NSEL):
                for part in range(2):
                    abuf[part * BS : (part + 1) * BS, i * BS : (i + 1) * BS] = strips[j][
                        ancestors[0, i], part
                    ]
            acc = jnp.dot(
                abuf[...], lbuf[...].reshape(NSEL * BS, 2 * S), preferred_element_type=F32
            )
            real = acc[:BS, :S] - acc[BS:, S:]
            imag = acc[:BS, S:] + acc[BS:, :S]
            chosen = jnp.int32(0)
            for i in range(NSEL):
                chosen += jnp.where(ancestors[0, i] == row * COLS + rb * 4 + depth, 1, 0)
            keep = lax.broadcast_in_dim(chosen, (BS, S), ()) > 0
            real = jnp.where(keep, real, 0.0)
            imag = jnp.where(keep, imag, 0.0)
            for q in range(4):
                lanes = slice(q * BS, (q + 1) * BS)
                ysend[q, rb] = jnp.concatenate([real[:, lanes], imag[:, lanes]], axis=1).astype(BF)
            for k in (2, 1, 3):
                r = up(k)
                remote(
                    ysend.at[r, rb],
                    yrecv.at[row, rb],
                    y_send.at[j, k],
                    y_recv.at[row, rb],
                    (pole, r, col),
                ).start()
            yrecv[row, rb] = ysend[row, rb]
            target = (column_send, column_out)[j]
            target[:, 0, :] = -real
            target[:, 1, :] = -imag
            if j == 0:
                remote(column_send, column_out, c_send, c_recv, (pole, row, facing)).start()
            share = -(weight_real * imag + weight_imag * real)
            columns.append(
                jnp.concatenate([share[:, q * BS : (q + 1) * BS] for q in range(4)], axis=0)
            )
        first = lax.broadcast_in_dim(works, columns[0].shape, ()) == 1
        share = jnp.concatenate(
            [
                jnp.where(first, columns[0], columns[1]),
                jnp.where(first, columns[1], columns[0]),
            ],
            axis=0,
        )
        high = share.astype(BF)
        low = (share - high.astype(F32)).astype(BF)
        tiles = jnp.dot(
            pick[...], jnp.concatenate([high, low], axis=1), preferred_element_type=F32
        )
        tiles = tiles[:, :BS] + tiles[:, BS:]
        tsend[...] = tiles.astype(BF).reshape(GRID, 32, BS)

        def send_tiles(k, carry):
            to, device = to_position(k)
            remote(tsend.at[to], trecv.at[source], t_send, t_recv, device).start()
            return carry

        lax.fori_loop(1, GRID, send_tiles, 0)
        trecv[source] = tsend[me]

        for k in (1, 3, 2):
            for rb in range(2):
                came(ysend.at[0, 0], y_recv.at[up(k), rb])
        mixed = jnp.dot(
            left[...], yrecv[...].reshape(8 * BS, 2 * BS), preferred_element_type=F32
        )
        diag_real = mixed[:S, :BS] - mixed[S:, BS:]
        diag_imag = mixed[:S, BS:] + mixed[S:, :BS]
        dsend[...] = (
            jnp.concatenate([diag_real, diag_imag], axis=1)
            .astype(BF)
            .reshape(GRID, S // GRID, 2 * BS)
        )

        def send_diag(k, carry):
            to, device = to_position(k)
            remote(dsend.at[to], drecv.at[source], d_send, d_recv, device).start()
            return carry

        lax.fori_loop(1, GRID, send_diag, 0)
        drecv[source] = dsend[me]

    def arrivals(ref, recv):
        @pl.when(active)
        def _():
            came(ref.at[pl.ds(0, GRID // 2 - 1)], recv)

        @pl.when(jnp.logical_not(active))
        def _():
            came(ref, recv)

    arrivals(trecv, t_recv)
    total = jnp.sum(trecv[...].astype(F32), axis=0)
    psend[...] = total.reshape(POLES, 8, BS)
    for k in range(1, POLES):
        p = (pole + k) % POLES
        remote(psend.at[p], precv.at[pole], p_send.at[k], p_recv.at[pole], (p, row, col)).start()
    precv[pole] = psend[pole]

    arrivals(drecv, d_recv)
    dreal, dimag = [], []
    for q in range(4):
        quarter = jnp.sum(drecv[q * 4 : (q + 1) * 4].astype(F32), axis=0)
        dreal.append(quarter[:, :BS])
        dimag.append(quarter[:, BS:])
    dreal = jnp.concatenate(dreal, axis=1) + dinv[:, 0, :]
    dimag = jnp.concatenate(dimag, axis=1) + dinv[:, 1, :]
    qsend[...] = weight_real * dimag + weight_imag * dreal
    for k in range(1, POLES):
        p = (pole + k) % POLES
        remote(qsend, qrecv.at[pole], q_send.at[k], q_recv.at[pole], (p, row, col)).start()
    qrecv[pole] = qsend[...]
    diag_out[:, 0, :] = dreal
    diag_out[:, 1, :] = dimag
    for k in range(1, POLES):
        p = (pole + k) % POLES
        came(psend.at[0], p_recv.at[p])
    tile_out[...] = jnp.sum(precv[...], axis=0)

    @pl.when(jnp.logical_not(active))
    def _():
        sent(lbuf.at[0, pl.ds(0, LROWS)], l_send.at[0])
        sent(owner.at[0], o_send)
        for n in range(8):
            sent(first_strips.at[pl.ds(0, 4)], g_send.at[n])
        came(column_out, c_recv)

    @pl.when(active)
    def _():
        for n in range(22):
            sent(lbuf.at[0, pl.ds(0, LROWS)], l_send.at[n])
        for n in range(16):
            sent(lbuf.at[0, pl.ds(0, HALF)], h_send.at[n])
        for n in range(6):
            sent(first_strips.at[pl.ds(0, 4)], g_send.at[n])
        for j in range(2):
            for k in (1, 2, 3):
                sent(ysend.at[0, 0], y_send.at[j, k])
        sent(column_send, c_send)
        sent(tsend.at[pl.ds(0, GRID - 1)], t_send)
        sent(dsend.at[pl.ds(0, GRID - 1)], d_send)

    for k in range(1, POLES):
        sent(psend.at[0], p_send.at[k])
        sent(qsend, q_send.at[k])
    for k in range(1, POLES):
        p = (pole + k) % POLES
        came(qsend, q_recv.at[p])
    density_out[:, 0, :] = jnp.sum(qrecv[...], axis=0)


def hand_out(*refs):
    done = refs[8]
    copies = [pltpu.make_async_copy(refs[k], refs[4 + k], done.at[k]) for k in range(4)]
    for copy in copies:
        copy.start()
    for copy in copies:
        copy.wait()


def body(inverse, factor, dinv, ancestors, owner, weight_table, pole_slot):
    vmem = pl.BlockSpec(memory_space=pltpu.VMEM)
    hbm = pl.BlockSpec(memory_space=pl.ANY)
    dma = pltpu.SemaphoreType.DMA
    column, diag, density, tile = pl.pallas_call(
        kernel,
        name="supernode",
        out_shape=(
            pltpu.VMEM((BS, 2, S), F32),
            pltpu.VMEM((S // GRID, 2, S), F32),
            pltpu.VMEM((S // GRID, 1, S), F32),
            pltpu.VMEM((8, BS), F32),
        ),
        in_specs=[pl.BlockSpec(memory_space=pltpu.HBM)] * 6 + [pl.BlockSpec(memory_space=pltpu.SMEM)],
        out_specs=(vmem,) * 4,
        scratch_shapes=[
            pltpu.VMEM((NSEL, BS, 2 * S), BF),
            pltpu.VMEM((COLS * 4, 2, BS, BS), BF),
            pltpu.VMEM((COLS * 4, 2, BS, BS), BF),
            pltpu.VMEM((2 * BS, NSEL * BS), BF),
            pltpu.VMEM((2 * S, 8 * BS), BF),
            pltpu.VMEM((BS, 2, S), F32),
            pltpu.VMEM((S // GRID, 2, S), F32),
            pltpu.VMEM((2, 1, 64), jnp.int32),
            pltpu.SMEM((1, NSEL), jnp.int32),
            pltpu.SMEM((2, NWEIGHT), F32),
            pltpu.VMEM((4, 2, BS, 2 * BS), BF),
            pltpu.VMEM((4, 2, BS, 2 * BS), BF),
            pltpu.VMEM((GRID, S // GRID, 2 * BS), BF),
            pltpu.VMEM((GRID // 2, S // GRID, 2 * BS), BF),
            pltpu.VMEM((1024, 1024), BF),
            pltpu.VMEM((GRID, 32, BS), BF),
            pltpu.VMEM((GRID // 2, 32, BS), BF),
            pltpu.VMEM((POLES, 8, BS), F32),
            pltpu.VMEM((POLES, 8, BS), F32),
            pltpu.VMEM((S // GRID, S), F32),
            pltpu.VMEM((POLES, S // GRID, S), F32),
            dma((8,)),
            dma((22,)),
            dma((GRID,)),
            dma((16,)),
            dma((2, COLS)),
            dma((8,)),
            dma((2, COLS)),
            dma,
            dma,
            dma,
            dma,
            dma((2, 4)),
            dma((4, 2)),
            dma,
            dma,
            dma,
            dma,
            dma((POLES,)),
            dma((POLES,)),
            dma((POLES,)),
            dma((POLES,)),
        ],
        compiler_params=pltpu.CompilerParams(
            collective_id=0, has_side_effects=True, vmem_limit_bytes=56 << 20
        ),
    )(
        *(
            pltpu.with_memory_space_constraint(x, pltpu.HBM)
            for x in (
                inverse.reshape(2, 1024, 512),
                factor.reshape(LROWS, 2 * S),
                dinv.reshape(S // GRID, 2, S),
                ancestors,
                owner.reshape(1, 64),
                weight_table,
            )
        ),
        pole_slot,
    )
    column, diag, density, tile = pl.pallas_call(
        hand_out,
        name="hand_out",
        out_shape=tuple(jax.ShapeDtypeStruct(x.shape, F32) for x in (column, diag, density, tile)),
        in_specs=[vmem] * 4,
        out_specs=(hbm,) * 4,
        scratch_shapes=[dma((4,))],
        compiler_params=pltpu.CompilerParams(vmem_limit_bytes=1 << 20),
    )(column, diag, density, tile)
    return (
        column.reshape(BS, 1, 1, 2, S),
        diag.reshape(S // GRID, 1, 1, 2, S),
        density,
        tile.reshape(1, 8, BS),
    )


def solution(mesh):
    grid = ("row", "col")
    in_specs = (
        P("pole", None, "row", "col"),
        P("pole", None, grid, None),
        P(grid, "pole", None, None, None),
        P(),
        P(grid, None),
        P(),
        P("pole"),
    )
    out_specs = (
        P(grid, "pole", None, None, None),
        P(grid, "pole", None, None, None),
        P(grid, None, None),
        P(("pole", "row", "col"), None, None),
    )
    return jax.shard_map(body, mesh=mesh, in_specs=in_specs, out_specs=out_specs, check_vma=False)
```

```python
import jax
import jax.numpy as jnp
from jax import lax
from jax.experimental import pallas as pl
from jax.experimental.pallas import tpu as pltpu
from jax.sharding import PartitionSpec as P

S = 512
BS = 128
NSEL = 16
NWEIGHT = 16
ROWS = 4
COLS = 8
POLES = 4
GRID = ROWS * COLS
LROWS = NSEL * BS // GRID
HALF = LROWS // 2
MESH = pl.DeviceIdType.MESH
BF = jnp.bfloat16
F32 = jnp.float32


def kernel(
    inverse,
    factor,
    dinv_in,
    ancestors_in,
    owner_in,
    table_in,
    slot,
    column_out,
    diag_out,
    density_out,
    tile_out,
    lbuf,
    first_strips,
    second_strips,
    relay,
    abuf,
    left,
    column_send,
    dinv,
    owner,
    ancestors,
    table,
    ysend,
    yrecv,
    dsend,
    drecv,
    pick,
    tsend,
    trecv,
    psend,
    precv,
    qsend,
    qrecv,
    local_sem,
    l_send,
    l_recv,
    h_send,
    h_recv,
    g_send,
    g_recv,
    r_send,
    s_recv,
    o_send,
    o_recv,
    c_send,
    c_recv,
    y_send,
    y_recv,
    d_send,
    d_recv,
    t_send,
    t_recv,
    p_send,
    p_recv,
    q_send,
    q_recv,
):
    pole, row, col = lax.axis_index("pole"), lax.axis_index("row"), lax.axis_index("col")
    side, depth = col // 4, col % 4
    me = row * COLS + col
    works = pole % 2
    active = side == works
    facing = (1 - side) * 4 + depth
    source = row * 4 + depth
    turns = (1 - works, works)
    strips = (first_strips, second_strips)

    def at_depth(s, dz):
        return s * 4 + (depth + dz) % 4

    def up(k):
        return (row + k) % ROWS

    def remote(src, dst, send, recv, to):
        return pltpu.make_async_remote_copy(
            src_ref=src,
            dst_ref=dst,
            send_sem=send,
            recv_sem=recv,
            device_id=to,
            device_id_type=MESH,
        )

    here = (pole, row, col)

    def sent(ref, send):
        remote(ref, ref, send, q_recv.at[0], here).wait_send()

    def came(ref, recv):
        remote(ref, ref, q_send.at[0], recv, here).wait_recv()

    own_factor = pltpu.make_async_copy(
        factor, lbuf.at[me // 2, pl.ds((me % 2) * LROWS, LROWS)], local_sem.at[0]
    )
    own_factor.start()
    small = [
        pltpu.make_async_copy(source, target, local_sem.at[2 + n])
        for n, (source, target) in enumerate(
            (
                (owner_in, owner.at[side]),
                (ancestors_in, ancestors),
                (table_in, table),
                (dinv_in, dinv),
            )
        )
    ]
    for copy in small:
        copy.start()

    def piece(rb, z, k):
        return inverse.at[:, pl.ds((rb * 4 + z) * BS, BS), pl.ds(k * BS, BS)]

    @pl.when(active)
    def _():
        for j, rb in enumerate(turns):
            for k in range(4):
                pltpu.make_async_copy(
                    piece(rb, depth, k), strips[j].at[col * 4 + k], local_sem.at[6 * j + 1]
                ).start()

    barrier = pltpu.get_barrier_semaphore()
    others = [(ds, dz) for ds in (0, 1) for dz in (0, 1, 3, 2) if (ds, dz) != (0, 0)]
    for ds, dz in others:
        c = ((side + ds) % 2) * 4 + (depth + dz) % 4
        pl.semaphore_signal(barrier, inc=1, device_id=(pole, row, c), device_id_type=MESH)
    for k in (1, 3, 2):
        pl.semaphore_signal(barrier, inc=1, device_id=(pole, up(k), col), device_id_type=MESH)
    for k in range(1, POLES):
        pl.semaphore_signal(
            barrier, inc=1, device_id=((pole + k) % POLES, row, col), device_id_type=MESH
        )
    pl.semaphore_wait(barrier, len(others) + ROWS - 1 + POLES - 1)
    own_factor.wait()
    for copy in small:
        copy.wait()

    def block(r, c):
        return lbuf.at[r * 4 + c // 2, pl.ds((c % 2) * LROWS, LROWS)]

    def half(r, c, part):
        return lbuf.at[r * 4 + c // 2, pl.ds((c % 2) * LROWS + part * HALF, HALF)]

    def send_strip(n, j, z):
        for k in range(4):
            remote(
                piece(turns[j], z, k),
                strips[j].at[col * 4 + k],
                g_send.at[n],
                g_recv.at[j, col],
                (pole, row, works * 4 + z),
            ).start()

    @pl.when(jnp.logical_not(active))
    def _():
        remote(
            block(row, col), block(row, col), l_send.at[0], l_recv.at[me], (pole, row, facing)
        ).start()
        remote(owner.at[side], owner.at[side], o_send, o_recv, (pole, row, facing)).start()
        for j in range(2):
            for i, dz in enumerate((1, 3, 2, 0)):
                z = (depth + dz) % 4
                for k in range(4):
                    remote(
                        piece(turns[j], z, k),
                        relay.at[j, i, k] if dz else strips[j].at[col * 4 + k],
                        g_send.at[4 * j + i],
                        s_recv.at[j, i] if dz else g_recv.at[j, col],
                        (pole, row, facing),
                    ).start()

    weight_real = table[0, slot[0]]
    weight_imag = table[1, slot[0]]

    def to_position(k):
        to = (me + k) % GRID
        return to, (pole, to // COLS, to % COLS)

    @pl.when(active)
    def _():
        count = [0]

        def send_block(r, c, to):
            k = count[0]
            count[0] += 1
            remote(
                block(r, c), block(r, c), l_send.at[k], l_recv.at[r * COLS + c], to
            ).start()

        def send_half(r, c, part, k, to):
            remote(
                half(r, c, part), half(r, c, part), h_send.at[k], h_recv.at[part, c], to
            ).start()

        def wait_block(r, c):
            came(block(r, c), l_recv.at[r * COLS + c])

        def along_rows(c):
            send_block(row, c, (pole, up(1), col))
            send_block(row, c, (pole, up(3), col))

        def pass_on(c):
            k = passed[0]
            passed[0] += 2
            wait_block(up(3), c)
            send_half(up(3), c, 0, k, (pole, up(1), col))
            wait_block(up(1), c)
            send_half(up(1), c, 1, k + 1, (pole, up(3), col))

        def in_plane(c):
            for dz in (1, 3, 2):
                send_block(row, c, (pole, row, at_depth(side, dz)))
            along_rows(c)

        def arrived_in_plane(c):
            wait_block(row, c)
            along_rows(c)

        def forward(j, i):
            came(relay.at[j, i], s_recv.at[j, i])
            remote(
                relay.at[j, i],
                strips[j].at[pl.ds(facing * 4, 4)],
                r_send.at[j, i],
                g_recv.at[j, facing],
                (pole, row, at_depth(side, (1, 3, 2)[i])),
            ).start()

        def send_own(j, i):
            send_strip(3 * j + i, j, (depth + (1, 3, 2)[i]) % 4)

        passed = [0]
        order = [col, facing]
        for dz in (1, 3, 2):
            order += [at_depth(side, dz), at_depth(1 - side, dz)]
        in_plane(col)
        send_own(0, 0)
        send_own(0, 1)
        wait_block(row, facing)
        in_plane(facing)
        arrived_in_plane(order[2])
        arrived_in_plane(order[4])
        forward(0, 0)
        forward(0, 1)
        send_own(0, 2)
        for k in (3, 5, 6, 7):
            arrived_in_plane(order[k])
        forward(0, 2)
        send_own(1, 0)
        send_own(1, 1)
        for k in (0, 1, 2, 4):
            pass_on(order[k])
        forward(1, 0)
        send_own(1, 2)
        for k in (3, 5, 6, 7):
            pass_on(order[k])
        forward(1, 1)

        came(owner.at[0], o_recv)
        lane = lax.broadcasted_iota(jnp.int32, (64, 512), 1)
        owner_index = lax.broadcasted_iota(jnp.int32, (64, 512), 0)
        named = ((lane & 127) >> 3) * 4 + (lane >> 7)
        across = lax.broadcasted_iota(jnp.int32, (64, 64), 1)
        down = lax.broadcasted_iota(jnp.int32, (64, 64), 0)
        position = lax.broadcasted_iota(jnp.int32, (1024, 512), 0).astype(F32)
        for s in range(2):
            target = jnp.where(across == down, owner[s].astype(F32), 0.0)
            target = jnp.sum(target, axis=1, keepdims=True).astype(jnp.int32)
            target = ((target & 31) * 32 + (target >> 5) * 8).astype(F32)
            spread = jnp.where(named == owner_index, target, 0.0)
            key = jnp.sum(spread, axis=0, keepdims=True) + (lane[:1] & 7).astype(F32)
            pick[:, s * 512 : (s + 1) * 512] = jnp.where(position == key, 1.0, 0.0).astype(BF)

        forward(1, 2)
        for c in order:
            came(half(up(2), c, 0), h_recv.at[0, c])
            came(half(up(2), c, 1), h_recv.at[1, c])
        for r in range(4):
            for s in range(2):
                b = r * COLS + s * 4 + depth
                before = jnp.int32(0)
                for i in range(NSEL):
                    before += jnp.where(ancestors[0, i] < b, 1, 0)
                before = jnp.minimum(before, NSEL - 1)
                at = (2 * r + s) * BS
                left[:, at : at + BS] = lbuf[before].T

        shares = [None, None]
        columns = []
        for j, rb in enumerate(turns):
            for s in (0, 1):
                for dz in (1, 3, 2, 0):
                    c = at_depth(s, dz)

                    @pl.when(c != col)
                    def _():
                        came(strips[j].at[pl.ds(0, 4)], g_recv.at[j, c])

            own = strips[j].at[pl.ds(col * 4, 4)]
            pltpu.make_async_copy(own, own, local_sem.at[6 * j + 1]).wait()
            for i in range(NSEL):
                for part in range(2):
                    abuf[part * BS : (part + 1) * BS, i * BS : (i + 1) * BS] = strips[j][
                        ancestors[0, i], part
                    ]
            acc = jnp.dot(
                abuf[...], lbuf[...].reshape(NSEL * BS, 2 * S), preferred_element_type=F32
            )
            real = acc[:BS, :S] - acc[BS:, S:]
            imag = acc[:BS, S:] + acc[BS:, :S]
            chosen = jnp.int32(0)
            for i in range(NSEL):
                chosen += jnp.where(ancestors[0, i] == row * COLS + rb * 4 + depth, 1, 0)
            keep = lax.broadcast_in_dim(chosen, (BS, S), ()) > 0
            real = jnp.where(keep, real, 0.0)
            imag = jnp.where(keep, imag, 0.0)
            for q in range(4):
                lanes = slice(q * BS, (q + 1) * BS)
                ysend[q, rb] = jnp.concatenate([real[:, lanes], imag[:, lanes]], axis=1).astype(BF)
            for k in (2, 1, 3):
                r = up(k)
                remote(
                    ysend.at[r, rb],
                    yrecv.at[row, rb],
                    y_send.at[j, k],
                    y_recv.at[row, rb],
                    (pole, r, col),
                ).start()
            yrecv[row, rb] = ysend[row, rb]
            target = (column_send, column_out)[j]
            target[:, 0, :] = -real
            target[:, 1, :] = -imag
            if j == 0:
                remote(column_send, column_out, c_send, c_recv, (pole, row, facing)).start()
            share = -(weight_real * imag + weight_imag * real)
            columns.append(
                jnp.concatenate([share[:, q * BS : (q + 1) * BS] for q in range(4)], axis=0)
            )
        first = lax.broadcast_in_dim(works, columns[0].shape, ()) == 1
        share = jnp.concatenate(
            [
                jnp.where(first, columns[0], columns[1]),
                jnp.where(first, columns[1], columns[0]),
            ],
            axis=0,
        )
        high = share.astype(BF)
        low = (share - high.astype(F32)).astype(BF)
        tiles = jnp.dot(
            pick[...], jnp.concatenate([high, low], axis=1), preferred_element_type=F32
        )
        tiles = tiles[:, :BS] + tiles[:, BS:]
        tsend[...] = tiles.astype(BF).reshape(GRID, 32, BS)

        def send_tiles(k, carry):
            to, device = to_position(k)
            remote(tsend.at[to], trecv.at[source], t_send, t_recv, device).start()
            return carry

        lax.fori_loop(1, GRID, send_tiles, 0)
        trecv[source] = tsend[me]

        for k in (1, 3, 2):
            for rb in range(2):
                came(ysend.at[0, 0], y_recv.at[up(k), rb])
        mixed = jnp.dot(
            left[...], yrecv[...].reshape(8 * BS, 2 * BS), preferred_element_type=F32
        )
        diag_real = mixed[:S, :BS] - mixed[S:, BS:]
        diag_imag = mixed[:S, BS:] + mixed[S:, :BS]
        dsend[...] = (
            jnp.concatenate([diag_real, diag_imag], axis=1)
            .astype(BF)
            .reshape(GRID, S // GRID, 2 * BS)
        )

        def send_diag(k, carry):
            to, device = to_position(k)
            remote(dsend.at[to], drecv.at[source], d_send, d_recv, device).start()
            return carry

        lax.fori_loop(1, GRID, send_diag, 0)
        drecv[source] = dsend[me]

    def arrivals(ref, recv):
        @pl.when(active)
        def _():
            came(ref.at[pl.ds(0, GRID // 2 - 1)], recv)

        @pl.when(jnp.logical_not(active))
        def _():
            came(ref, recv)

    arrivals(trecv, t_recv)
    total = jnp.sum(trecv[...].astype(F32), axis=0)
    psend[...] = total.reshape(POLES, 8, BS)
    for k in range(1, POLES):
        p = (pole + k) % POLES
        remote(psend.at[p], precv.at[pole], p_send.at[k], p_recv.at[pole], (p, row, col)).start()
    precv[pole] = psend[pole]

    arrivals(drecv, d_recv)
    dreal, dimag = [], []
    for q in range(4):
        quarter = jnp.sum(drecv[q * 4 : (q + 1) * 4].astype(F32), axis=0)
        dreal.append(quarter[:, :BS])
        dimag.append(quarter[:, BS:])
    dreal = jnp.concatenate(dreal, axis=1) + dinv[:, 0, :]
    dimag = jnp.concatenate(dimag, axis=1) + dinv[:, 1, :]
    qsend[...] = weight_real * dimag + weight_imag * dreal
    for k in range(1, POLES):
        p = (pole + k) % POLES
        remote(qsend, qrecv.at[pole], q_send.at[k], q_recv.at[pole], (p, row, col)).start()
    qrecv[pole] = qsend[...]
    diag_out[:, 0, :] = dreal
    diag_out[:, 1, :] = dimag
    for k in range(1, POLES):
        p = (pole + k) % POLES
        came(psend.at[0], p_recv.at[p])
    tile_out[...] = jnp.sum(precv[...], axis=0)

    @pl.when(jnp.logical_not(active))
    def _():
        sent(lbuf.at[0, pl.ds(0, LROWS)], l_send.at[0])
        sent(owner.at[0], o_send)
        for n in range(8):
            sent(first_strips.at[pl.ds(0, 4)], g_send.at[n])
        came(column_out, c_recv)

    @pl.when(active)
    def _():
        for n in range(22):
            sent(lbuf.at[0, pl.ds(0, LROWS)], l_send.at[n])
        for n in range(16):
            sent(lbuf.at[0, pl.ds(0, HALF)], h_send.at[n])
        for n in range(6):
            sent(first_strips.at[pl.ds(0, 4)], g_send.at[n])
        for j in range(2):
            for i in range(3):
                sent(relay.at[j, i], r_send.at[j, i])
            for k in (1, 2, 3):
                sent(ysend.at[0, 0], y_send.at[j, k])
        sent(column_send, c_send)
        sent(tsend.at[pl.ds(0, GRID - 1)], t_send)
        sent(dsend.at[pl.ds(0, GRID - 1)], d_send)

    for k in range(1, POLES):
        sent(psend.at[0], p_send.at[k])
        sent(qsend, q_send.at[k])
    for k in range(1, POLES):
        p = (pole + k) % POLES
        came(qsend, q_recv.at[p])
    density_out[:, 0, :] = jnp.sum(qrecv[...], axis=0)


def hand_out(*refs):
    done = refs[8]
    copies = [pltpu.make_async_copy(refs[k], refs[4 + k], done.at[k]) for k in range(4)]
    for copy in copies:
        copy.start()
    for copy in copies:
        copy.wait()


def body(inverse, factor, dinv, ancestors, owner, weight_table, pole_slot):
    vmem = pl.BlockSpec(memory_space=pltpu.VMEM)
    hbm = pl.BlockSpec(memory_space=pl.ANY)
    dma = pltpu.SemaphoreType.DMA
    column, diag, density, tile = pl.pallas_call(
        kernel,
        name="supernode",
        out_shape=(
            pltpu.VMEM((BS, 2, S), F32),
            pltpu.VMEM((S // GRID, 2, S), F32),
            pltpu.VMEM((S // GRID, 1, S), F32),
            pltpu.VMEM((8, BS), F32),
        ),
        in_specs=[pl.BlockSpec(memory_space=pltpu.HBM)] * 6 + [pl.BlockSpec(memory_space=pltpu.SMEM)],
        out_specs=(vmem,) * 4,
        scratch_shapes=[
            pltpu.VMEM((NSEL, BS, 2 * S), BF),
            pltpu.VMEM((COLS * 4, 2, BS, BS), BF),
            pltpu.VMEM((COLS * 4, 2, BS, BS), BF),
            pltpu.VMEM((2, 3, 4, 2, BS, BS), BF),
            pltpu.VMEM((2 * BS, NSEL * BS), BF),
            pltpu.VMEM((2 * S, 8 * BS), BF),
            pltpu.VMEM((BS, 2, S), F32),
            pltpu.VMEM((S // GRID, 2, S), F32),
            pltpu.VMEM((2, 1, 64), jnp.int32),
            pltpu.SMEM((1, NSEL), jnp.int32),
            pltpu.SMEM((2, NWEIGHT), F32),
            pltpu.VMEM((4, 2, BS, 2 * BS), BF),
            pltpu.VMEM((4, 2, BS, 2 * BS), BF),
            pltpu.VMEM((GRID, S // GRID, 2 * BS), BF),
            pltpu.VMEM((GRID // 2, S // GRID, 2 * BS), BF),
            pltpu.VMEM((1024, 1024), BF),
            pltpu.VMEM((GRID, 32, BS), BF),
            pltpu.VMEM((GRID // 2, 32, BS), BF),
            pltpu.VMEM((POLES, 8, BS), F32),
            pltpu.VMEM((POLES, 8, BS), F32),
            pltpu.VMEM((S // GRID, S), F32),
            pltpu.VMEM((POLES, S // GRID, S), F32),
            dma((8,)),
            dma((22,)),
            dma((GRID,)),
            dma((16,)),
            dma((2, COLS)),
            dma((8,)),
            dma((2, COLS)),
            dma((2, 3)),
            dma((2, 3)),
            dma,
            dma,
            dma,
            dma,
            dma((2, 4)),
            dma((4, 2)),
            dma,
            dma,
            dma,
            dma,
            dma((POLES,)),
            dma((POLES,)),
            dma((POLES,)),
            dma((POLES,)),
        ],
        compiler_params=pltpu.CompilerParams(
            collective_id=0, has_side_effects=True, vmem_limit_bytes=56 << 20
        ),
    )(
        *(
            pltpu.with_memory_space_constraint(x, pltpu.HBM)
            for x in (
                inverse.reshape(2, 1024, 512),
                factor.reshape(LROWS, 2 * S),
                dinv.reshape(S // GRID, 2, S),
                ancestors,
                owner.reshape(1, 64),
                weight_table,
            )
        ),
        pole_slot,
    )
    column, diag, density, tile = pl.pallas_call(
        hand_out,
        name="hand_out",
        out_shape=tuple(jax.ShapeDtypeStruct(x.shape, F32) for x in (column, diag, density, tile)),
        in_specs=[vmem] * 4,
        out_specs=(hbm,) * 4,
        scratch_shapes=[dma((4,))],
        compiler_params=pltpu.CompilerParams(vmem_limit_bytes=1 << 20),
    )(column, diag, density, tile)
    return (
        column.reshape(BS, 1, 1, 2, S),
        diag.reshape(S // GRID, 1, 1, 2, S),
        density,
        tile.reshape(1, 8, BS),
    )


def solution(mesh):
    grid = ("row", "col")
    in_specs = (
        P("pole", None, "row", "col"),
        P("pole", None, grid, None),
        P(grid, "pole", None, None, None),
        P(),
        P(grid, None),
        P(),
        P("pole"),
    )
    out_specs = (
        P(grid, "pole", None, None, None),
        P(grid, "pole", None, None, None),
        P(grid, None, None),
        P(("pole", "row", "col"), None, None),
    )
    return jax.shard_map(body, mesh=mesh, in_specs=in_specs, out_specs=out_specs, check_vma=False)
```

```python
import jax
import jax.numpy as jnp
from jax import lax
from jax.experimental import pallas as pl
from jax.experimental.pallas import tpu as pltpu
from jax.sharding import PartitionSpec as P

S = 512
BS = 128
NSEL = 16
NWEIGHT = 16
ROWS = 4
COLS = 8
POLES = 4
GRID = ROWS * COLS
LROWS = NSEL * BS // GRID
HALF = LROWS // 2
MESH = pl.DeviceIdType.MESH
BF = jnp.bfloat16
F32 = jnp.float32


def kernel(
    inverse,
    factor,
    dinv_in,
    ancestors_in,
    owner_in,
    table_in,
    slot,
    column_out,
    diag_out,
    density_out,
    tile_out,
    lbuf,
    first_strips,
    second_strips,
    relay,
    spread,
    abuf,
    left,
    column_send,
    dinv,
    owner,
    ancestors,
    table,
    ysend,
    yrecv,
    dsend,
    drecv,
    pick,
    tsend,
    trecv,
    psend,
    precv,
    qsend,
    qrecv,
    beside_sem,
    local_sem,
    l_send,
    l_recv,
    h_send,
    h_recv,
    g_send,
    g_recv,
    r_send,
    s_recv,
    o_send,
    o_recv,
    c_send,
    c_recv,
    y_send,
    y_recv,
    d_send,
    d_recv,
    t_send,
    t_recv,
    p_send,
    p_recv,
    q_send,
    q_recv,
):
    pole, row, col = lax.axis_index("pole"), lax.axis_index("row"), lax.axis_index("col")
    side, depth = col // 4, col % 4
    me = row * COLS + col
    works = pole % 2
    active = side == works
    facing = (1 - side) * 4 + depth
    source = row * 4 + depth
    turns = (1 - works, works)
    strips = (first_strips, second_strips)

    def at_depth(s, dz):
        return s * 4 + (depth + dz) % 4

    def up(k):
        return (row + k) % ROWS

    def remote(src, dst, send, recv, to):
        return pltpu.make_async_remote_copy(
            src_ref=src,
            dst_ref=dst,
            send_sem=send,
            recv_sem=recv,
            device_id=to,
            device_id_type=MESH,
        )

    here = (pole, row, col)

    def sent(ref, send):
        remote(ref, ref, send, q_recv.at[0], here).wait_send()

    def came(ref, recv):
        remote(ref, ref, q_send.at[0], recv, here).wait_recv()

    own_factor = pltpu.make_async_copy(
        factor, lbuf.at[me // 2, pl.ds((me % 2) * LROWS, LROWS)], local_sem.at[0]
    )
    own_factor.start()
    small = [
        pltpu.make_async_copy(source, target, local_sem.at[2 + n])
        for n, (source, target) in enumerate(
            (
                (owner_in, owner.at[side]),
                (ancestors_in, ancestors),
                (table_in, table),
                (dinv_in, dinv),
            )
        )
    ]
    for copy in small:
        copy.start()

    def piece(rb, z):
        return inverse.at[:, pl.ds((rb * 4 + z) * BS, BS)]

    @pl.when(active)
    def _():
        for j, rb in enumerate(turns):
            pltpu.make_async_copy(
                piece(rb, depth), strips[j].at[col], local_sem.at[6 * j + 1]
            ).start()

    barrier = pltpu.get_barrier_semaphore()
    beside = (((pole + 2) % POLES, row, facing), ((pole + 2) % POLES + 1 - 2 * works, row, facing))
    neighbours = [
        (pole, row, facing),
        (pole, row, at_depth(side, 1)),
        (pole, row, at_depth(side, 3)),
        (pole, up(1), col),
        (pole, up(3), col),
        (pole + 1 - 2 * works, row, col),
        *beside,
    ]
    for device in neighbours:
        pl.semaphore_signal(barrier, inc=1, device_id=device, device_id_type=MESH)
    pl.semaphore_wait(barrier, len(neighbours))
    for device in beside:
        pl.semaphore_signal(beside_sem, inc=1, device_id=device, device_id_type=MESH)
    own_factor.wait()
    for copy in small:
        copy.wait()

    def block(r, c):
        return lbuf.at[r * 4 + c // 2, pl.ds((c % 2) * LROWS, LROWS)]

    def half(r, c, part):
        return lbuf.at[r * 4 + c // 2, pl.ds((c % 2) * LROWS + part * HALF, HALF)]

    def send_strip(n, j, z):
        remote(
            piece(turns[j], z),
            strips[j].at[col],
            g_send.at[n],
            g_recv.at[j, col],
            (pole, row, works * 4 + z),
        ).start()

    @pl.when(jnp.logical_not(active))
    def _():
        remote(
            block(row, col), block(row, col), l_send.at[0], l_recv.at[me], (pole, row, facing)
        ).start()
        remote(owner.at[side], owner.at[side], o_send, o_recv, (pole, row, facing)).start()
        for j in range(2):
            for i, dz in enumerate((1, 3, 2, 0)):
                remote(
                    piece(turns[j], (depth + dz) % 4),
                    relay.at[j, i] if dz else strips[j].at[col],
                    g_send.at[4 * j + i],
                    s_recv.at[j, i] if dz else g_recv.at[j, col],
                    (pole, row, facing),
                ).start()

    weight_real = table[0, slot[0]]
    weight_imag = table[1, slot[0]]

    def send_all(src, dst, send, recv):
        far = [(dr, ds, dz) for dr in range(ROWS) for ds in range(2) for dz in range(4)]
        far.sort(key=lambda d: -(min(d[0], 4 - d[0]) + d[1] + min(d[2], 4 - d[2])))
        for dr, ds, dz in far[:-1]:
            c = at_depth((side + ds) % 2, dz)
            to = up(dr) * COLS + c
            remote(src.at[to], dst.at[source], send, recv, (pole, up(dr), c)).start()
        dst[source] = src[me]

    @pl.when(active)
    def _():
        count = [0]

        def send_block(r, c, to):
            k = count[0]
            count[0] += 1
            remote(
                block(r, c), block(r, c), l_send.at[k], l_recv.at[r * COLS + c], to
            ).start()

        def send_half(r, c, part, k, to):
            remote(
                half(r, c, part), half(r, c, part), h_send.at[k], h_recv.at[part, c], to
            ).start()

        def wait_block(r, c):
            came(block(r, c), l_recv.at[r * COLS + c])

        def along_rows(c):
            send_block(row, c, (pole, up(1), col))
            send_block(row, c, (pole, up(3), col))

        def pass_on(c):
            k = passed[0]
            passed[0] += 2
            wait_block(up(3), c)
            send_half(up(3), c, 0, k, (pole, up(1), col))
            wait_block(up(1), c)
            send_half(up(1), c, 1, k + 1, (pole, up(3), col))

        def in_plane(c, steps):
            for dz in steps:
                send_block(row, c, (pole, row, at_depth(side, dz)))

        def arrived_in_plane(c):
            wait_block(row, c)
            along_rows(c)

        def forward(j, i):
            came(relay.at[j, i], s_recv.at[j, i])
            remote(
                relay.at[j, i],
                strips[j].at[facing],
                r_send.at[j, i],
                g_recv.at[j, facing],
                (pole, row, at_depth(side, (1, 3, 2)[i])),
            ).start()

        def send_own(j, i):
            send_strip(3 * j + i, j, (depth + (1, 3, 2)[i]) % 4)

        passed = [0]
        order = [col, facing]
        for dz in (1, 3, 2):
            order += [at_depth(side, dz), at_depth(1 - side, dz)]
        in_plane(col, (1, 3))
        along_rows(col)
        send_own(0, 0)
        send_own(0, 1)
        arrived_in_plane(order[2])
        in_plane(col, (2,))
        wait_block(row, facing)
        in_plane(facing, (1, 3, 2))
        along_rows(facing)
        send_own(0, 2)
        arrived_in_plane(order[4])
        forward(0, 0)
        forward(0, 1)
        send_own(1, 0)
        send_own(1, 1)
        for k in (3, 5, 6, 7):
            arrived_in_plane(order[k])
        forward(0, 2)
        send_own(1, 2)
        for k in (0, 1, 2):
            pass_on(order[k])
        forward(1, 0)
        for k in (4, 3):
            pass_on(order[k])
        forward(1, 1)
        for k in (5, 6, 7):
            pass_on(order[k])

        came(owner.at[0], o_recv)
        lane = lax.broadcasted_iota(jnp.int32, (64, 512), 1)
        owner_index = lax.broadcasted_iota(jnp.int32, (64, 512), 0)
        named = ((lane & 127) >> 3) * 4 + (lane >> 7)
        across = lax.broadcasted_iota(jnp.int32, (64, 64), 1)
        down = lax.broadcasted_iota(jnp.int32, (64, 64), 0)
        position = lax.broadcasted_iota(jnp.int32, (1024, 512), 0).astype(F32)
        for s in range(2):
            target = jnp.where(across == down, owner[s].astype(F32), 0.0)
            target = jnp.sum(target, axis=1, keepdims=True).astype(jnp.int32)
            target = ((target & 31) * 32 + (target >> 5) * 8).astype(F32)
            placed = jnp.where(named == owner_index, target, 0.0)
            key = jnp.sum(placed, axis=0, keepdims=True) + (lane[:1] & 7).astype(F32)
            pick[:, s * 512 : (s + 1) * 512] = jnp.where(position == key, 1.0, 0.0).astype(BF)

        forward(1, 2)
        for c in order:
            came(half(up(2), c, 0), h_recv.at[0, c])
            came(half(up(2), c, 1), h_recv.at[1, c])
        for r in range(4):
            for s in range(2):
                b = r * COLS + s * 4 + depth
                before = jnp.int32(0)
                for i in range(NSEL):
                    before += jnp.where(ancestors[0, i] < b, 1, 0)
                before = jnp.minimum(before, NSEL - 1)
                at = (2 * r + s) * BS
                left[:, at : at + BS] = lbuf[before].T

        shares = [None, None]
        columns = []
        for j, rb in enumerate(turns):
            for ds, dz in ((0, 0), (0, 1), (0, 3), (0, 2), (1, 1), (1, 3), (1, 0), (1, 2)):
                c = at_depth((side + ds) % 2, dz)
                if (ds, dz) == (0, 0):
                    own = strips[j].at[c]
                    pltpu.make_async_copy(own, own, local_sem.at[6 * j + 1]).wait()
                else:
                    came(strips[j].at[0], g_recv.at[j, c])
                for part in range(2):
                    for k in range(4):
                        spread[c * 4 + k, part] = strips[j][c, part, :, k * BS : (k + 1) * BS]
            for i in range(NSEL):
                for part in range(2):
                    abuf[part * BS : (part + 1) * BS, i * BS : (i + 1) * BS] = spread[
                        ancestors[0, i], part
                    ]
            acc = jnp.dot(
                abuf[...], lbuf[...].reshape(NSEL * BS, 2 * S), preferred_element_type=F32
            )
            real = acc[:BS, :S] - acc[BS:, S:]
            imag = acc[:BS, S:] + acc[BS:, :S]
            chosen = jnp.int32(0)
            for i in range(NSEL):
                chosen += jnp.where(ancestors[0, i] == row * COLS + rb * 4 + depth, 1, 0)
            keep = lax.broadcast_in_dim(chosen, (BS, S), ()) > 0
            real = jnp.where(keep, real, 0.0)
            imag = jnp.where(keep, imag, 0.0)
            for q in range(4):
                lanes = slice(q * BS, (q + 1) * BS)
                ysend[q, rb] = jnp.concatenate([real[:, lanes], imag[:, lanes]], axis=1).astype(BF)
            for k in (2, 1, 3):
                r = up(k)
                remote(
                    ysend.at[r, rb],
                    yrecv.at[row, rb],
                    y_send.at[j, k],
                    y_recv.at[row, rb],
                    (pole, r, col),
                ).start()
            yrecv[row, rb] = ysend[row, rb]
            target = (column_send, column_out)[j]
            target[:, 0, :] = -real
            target[:, 1, :] = -imag
            if j == 0:
                remote(column_send, column_out, c_send, c_recv, (pole, row, facing)).start()
            share = -(weight_real * imag + weight_imag * real)
            columns.append(
                jnp.concatenate([share[:, q * BS : (q + 1) * BS] for q in range(4)], axis=0)
            )
        first = lax.broadcast_in_dim(works, columns[0].shape, ()) == 1
        share = jnp.concatenate(
            [
                jnp.where(first, columns[0], columns[1]),
                jnp.where(first, columns[1], columns[0]),
            ],
            axis=0,
        )
        high = share.astype(BF)
        low = (share - high.astype(F32)).astype(BF)
        tiles = jnp.dot(
            pick[...], jnp.concatenate([high, low], axis=1), preferred_element_type=F32
        )
        tiles = tiles[:, :BS] + tiles[:, BS:]
        tsend[...] = tiles.astype(BF).reshape(GRID, 32, BS)

        send_all(tsend, trecv, t_send, t_recv)

        for k in (1, 3, 2):
            for rb in range(2):
                came(ysend.at[0, 0], y_recv.at[up(k), rb])
        mixed = jnp.dot(
            left[...], yrecv[...].reshape(8 * BS, 2 * BS), preferred_element_type=F32
        )
        diag_real = mixed[:S, :BS] - mixed[S:, BS:]
        diag_imag = mixed[:S, BS:] + mixed[S:, :BS]
        dsend[...] = (
            jnp.concatenate([diag_real, diag_imag], axis=1)
            .astype(BF)
            .reshape(GRID, S // GRID, 2 * BS)
        )

        send_all(dsend, drecv, d_send, d_recv)

    def arrivals(ref, recv):
        @pl.when(active)
        def _():
            came(ref.at[pl.ds(0, GRID // 2 - 1)], recv)

        @pl.when(jnp.logical_not(active))
        def _():
            came(ref, recv)

    arrivals(trecv, t_recv)
    total = jnp.sum(trecv[...].astype(F32), axis=0)
    psend[...] = total.reshape(POLES, 8, BS)
    pl.semaphore_wait(beside_sem, len(beside))
    for k in range(1, POLES):
        p = (pole + k) % POLES
        remote(psend.at[p], precv.at[pole], p_send.at[k], p_recv.at[pole], (p, row, col)).start()
    precv[pole] = psend[pole]

    arrivals(drecv, d_recv)
    dreal, dimag = [], []
    for q in range(4):
        quarter = jnp.sum(drecv[q * 4 : (q + 1) * 4].astype(F32), axis=0)
        dreal.append(quarter[:, :BS])
        dimag.append(quarter[:, BS:])
    dreal = jnp.concatenate(dreal, axis=1) + dinv[:, 0, :]
    dimag = jnp.concatenate(dimag, axis=1) + dinv[:, 1, :]
    qsend[...] = weight_real * dimag + weight_imag * dreal
    for k in range(1, POLES):
        p = (pole + k) % POLES
        remote(qsend, qrecv.at[pole], q_send.at[k], q_recv.at[pole], (p, row, col)).start()
    qrecv[pole] = qsend[...]
    diag_out[:, 0, :] = dreal
    diag_out[:, 1, :] = dimag
    for k in range(1, POLES):
        p = (pole + k) % POLES
        came(psend.at[0], p_recv.at[p])
    tile_out[...] = jnp.sum(precv[...], axis=0)

    @pl.when(jnp.logical_not(active))
    def _():
        sent(lbuf.at[0, pl.ds(0, LROWS)], l_send.at[0])
        sent(owner.at[0], o_send)
        for n in range(8):
            sent(first_strips.at[0], g_send.at[n])
        came(column_out, c_recv)

    @pl.when(active)
    def _():
        for n in range(22):
            sent(lbuf.at[0, pl.ds(0, LROWS)], l_send.at[n])
        for n in range(16):
            sent(lbuf.at[0, pl.ds(0, HALF)], h_send.at[n])
        for n in range(6):
            sent(first_strips.at[0], g_send.at[n])
        for j in range(2):
            for i in range(3):
                sent(relay.at[j, i], r_send.at[j, i])
            for k in (1, 2, 3):
                sent(ysend.at[0, 0], y_send.at[j, k])
        sent(column_send, c_send)
        sent(tsend.at[pl.ds(0, GRID - 1)], t_send)
        sent(dsend.at[pl.ds(0, GRID - 1)], d_send)

    for k in range(1, POLES):
        sent(psend.at[0], p_send.at[k])
        sent(qsend, q_send.at[k])
    for k in range(1, POLES):
        p = (pole + k) % POLES
        came(qsend, q_recv.at[p])
    density_out[:, 0, :] = jnp.sum(qrecv[...], axis=0)


def hand_out(*refs):
    done = refs[8]
    copies = [pltpu.make_async_copy(refs[k], refs[4 + k], done.at[k]) for k in range(4)]
    for copy in copies:
        copy.start()
    for copy in copies:
        copy.wait()


def body(inverse, factor, dinv, ancestors, owner, weight_table, pole_slot):
    vmem = pl.BlockSpec(memory_space=pltpu.VMEM)
    hbm = pl.BlockSpec(memory_space=pl.ANY)
    dma = pltpu.SemaphoreType.DMA
    column, diag, density, tile = pl.pallas_call(
        kernel,
        name="supernode",
        out_shape=(
            pltpu.VMEM((BS, 2, S), F32),
            pltpu.VMEM((S // GRID, 2, S), F32),
            pltpu.VMEM((S // GRID, 1, S), F32),
            pltpu.VMEM((8, BS), F32),
        ),
        in_specs=[pl.BlockSpec(memory_space=pltpu.HBM)] * 6 + [pl.BlockSpec(memory_space=pltpu.SMEM)],
        out_specs=(vmem,) * 4,
        scratch_shapes=[
            pltpu.VMEM((NSEL, BS, 2 * S), BF),
            pltpu.VMEM((COLS, 2, BS, S), BF),
            pltpu.VMEM((COLS, 2, BS, S), BF),
            pltpu.VMEM((2, 3, 2, BS, S), BF),
            pltpu.VMEM((COLS * 4, 2, BS, BS), BF),
            pltpu.VMEM((2 * BS, NSEL * BS), BF),
            pltpu.VMEM((2 * S, 8 * BS), BF),
            pltpu.VMEM((BS, 2, S), F32),
            pltpu.VMEM((S // GRID, 2, S), F32),
            pltpu.VMEM((2, 1, 64), jnp.int32),
            pltpu.SMEM((1, NSEL), jnp.int32),
            pltpu.SMEM((2, NWEIGHT), F32),
            pltpu.VMEM((4, 2, BS, 2 * BS), BF),
            pltpu.VMEM((4, 2, BS, 2 * BS), BF),
            pltpu.VMEM((GRID, S // GRID, 2 * BS), BF),
            pltpu.VMEM((GRID // 2, S // GRID, 2 * BS), BF),
            pltpu.VMEM((1024, 1024), BF),
            pltpu.VMEM((GRID, 32, BS), BF),
            pltpu.VMEM((GRID // 2, 32, BS), BF),
            pltpu.VMEM((POLES, 8, BS), F32),
            pltpu.VMEM((POLES, 8, BS), F32),
            pltpu.VMEM((S // GRID, S), F32),
            pltpu.VMEM((POLES, S // GRID, S), F32),
            pltpu.SemaphoreType.REGULAR,
            dma((8,)),
            dma((22,)),
            dma((GRID,)),
            dma((16,)),
            dma((2, COLS)),
            dma((8,)),
            dma((2, COLS)),
            dma((2, 3)),
            dma((2, 3)),
            dma,
            dma,
            dma,
            dma,
            dma((2, 4)),
            dma((4, 2)),
            dma,
            dma,
            dma,
            dma,
            dma((POLES,)),
            dma((POLES,)),
            dma((POLES,)),
            dma((POLES,)),
        ],
        compiler_params=pltpu.CompilerParams(
            collective_id=0, has_side_effects=True, vmem_limit_bytes=56 << 20
        ),
    )(
        *(
            pltpu.with_memory_space_constraint(x, pltpu.HBM)
            for x in (
                inverse.reshape(2, 1024, 512),
                factor.reshape(LROWS, 2 * S),
                dinv.reshape(S // GRID, 2, S),
                ancestors,
                owner.reshape(1, 64),
                weight_table,
            )
        ),
        pole_slot,
    )
    column, diag, density, tile = pl.pallas_call(
        hand_out,
        name="hand_out",
        out_shape=tuple(jax.ShapeDtypeStruct(x.shape, F32) for x in (column, diag, density, tile)),
        in_specs=[vmem] * 4,
        out_specs=(hbm,) * 4,
        scratch_shapes=[dma((4,))],
        compiler_params=pltpu.CompilerParams(vmem_limit_bytes=1 << 20),
    )(column, diag, density, tile)
    return (
        column.reshape(BS, 1, 1, 2, S),
        diag.reshape(S // GRID, 1, 1, 2, S),
        density,
        tile.reshape(1, 8, BS),
    )


def solution(mesh):
    grid = ("row", "col")
    in_specs = (
        P("pole", None, "row", "col"),
        P("pole", None, grid, None),
        P(grid, "pole", None, None, None),
        P(),
        P(grid, None),
        P(),
        P("pole"),
    )
    out_specs = (
        P(grid, "pole", None, None, None),
        P(grid, "pole", None, None, None),
        P(grid, None, None),
        P(("pole", "row", "col"), None, None),
    )
    return jax.shard_map(body, mesh=mesh, in_specs=in_specs, out_specs=out_specs, check_vma=False)
```

```python
import jax
import jax.numpy as jnp
from jax import lax
from jax.experimental import pallas as pl
from jax.experimental.pallas import tpu as pltpu
from jax.sharding import PartitionSpec as P

S = 512
BS = 128
NSEL = 16
NWEIGHT = 16
ROWS = 4
COLS = 8
POLES = 4
GRID = ROWS * COLS
LROWS = NSEL * BS // GRID
HALF = LROWS // 2
MESH = pl.DeviceIdType.MESH
BF = jnp.bfloat16
F32 = jnp.float32


def kernel(
    inverse,
    factor,
    dinv_in,
    ancestors_in,
    owner_in,
    table_in,
    slot,
    column_out,
    diag_out,
    density_out,
    tile_out,
    lbuf,
    first_strips,
    second_strips,
    relay,
    spread,
    abuf,
    left,
    column_send,
    dinv,
    owner,
    ancestors,
    table,
    ysend,
    yrecv,
    dsend,
    drecv,
    pick,
    tsend,
    trecv,
    psend,
    precv,
    qsend,
    qrecv,
    beside_sem,
    local_sem,
    l_send,
    l_recv,
    h_send,
    h_recv,
    g_send,
    g_recv,
    r_send,
    s_recv,
    o_send,
    o_recv,
    c_send,
    c_recv,
    y_send,
    y_recv,
    d_send,
    d_recv,
    t_send,
    t_recv,
    p_send,
    p_recv,
    q_send,
    q_recv,
):
    pole, row, col = lax.axis_index("pole"), lax.axis_index("row"), lax.axis_index("col")
    side, depth = col // 4, col % 4
    me = row * COLS + col
    core = pole % 2
    works = 1 - core
    active = side == works
    facing = (1 - side) * 4 + depth
    source = row * 4 + depth
    turns = (1 - works, works)
    strips = (first_strips, second_strips)

    def at_depth(s, dz):
        return s * 4 + (depth + dz) % 4

    def up(k):
        return (row + k) % ROWS

    def remote(src, dst, send, recv, to):
        return pltpu.make_async_remote_copy(
            src_ref=src,
            dst_ref=dst,
            send_sem=send,
            recv_sem=recv,
            device_id=to,
            device_id_type=MESH,
        )

    here = (pole, row, col)

    def sent(ref, send):
        remote(ref, ref, send, q_recv.at[0], here).wait_send()

    def came(ref, recv):
        remote(ref, ref, q_send.at[0], recv, here).wait_recv()

    own_factor = pltpu.make_async_copy(
        factor, lbuf.at[me // 2, pl.ds((me % 2) * LROWS, LROWS)], local_sem.at[0]
    )
    own_factor.start()
    small = [
        pltpu.make_async_copy(source, target, local_sem.at[2 + n])
        for n, (source, target) in enumerate(
            (
                (owner_in, owner.at[side]),
                (ancestors_in, ancestors),
                (table_in, table),
                (dinv_in, dinv),
            )
        )
    ]
    for copy in small:
        copy.start()

    def piece(rb, z):
        return inverse.at[:, pl.ds((rb * 4 + z) * BS, BS)]

    @pl.when(active)
    def _():
        for j, rb in enumerate(turns):
            pltpu.make_async_copy(
                piece(rb, depth), strips[j].at[col], local_sem.at[6 * j + 1]
            ).start()

    barrier = pltpu.get_barrier_semaphore()
    beside = (((pole + 2) % POLES, row, facing), ((pole + 2) % POLES + 1 - 2 * core, row, facing))
    neighbours = [
        (pole, row, facing),
        (pole, row, at_depth(side, 1)),
        (pole, row, at_depth(side, 3)),
        (pole, up(1), col),
        (pole, up(3), col),
        (pole + 1 - 2 * core, row, col),
        *beside,
    ]
    for device in neighbours:
        pl.semaphore_signal(barrier, inc=1, device_id=device, device_id_type=MESH)
    pl.semaphore_wait(barrier, len(neighbours))
    for device in beside:
        pl.semaphore_signal(beside_sem, inc=1, device_id=device, device_id_type=MESH)
    own_factor.wait()
    for copy in small:
        copy.wait()

    def block(r, c):
        return lbuf.at[r * 4 + c // 2, pl.ds((c % 2) * LROWS, LROWS)]

    def half(r, c, part):
        return lbuf.at[r * 4 + c // 2, pl.ds((c % 2) * LROWS + part * HALF, HALF)]

    def send_strip(n, j, z):
        remote(
            piece(turns[j], z),
            strips[j].at[col],
            g_send.at[n],
            g_recv.at[j, col],
            (pole, row, works * 4 + z),
        ).start()

    @pl.when(jnp.logical_not(active))
    def _():
        remote(
            block(row, col), block(row, col), l_send.at[0], l_recv.at[me], (pole, row, facing)
        ).start()
        remote(owner.at[side], owner.at[side], o_send, o_recv, (pole, row, facing)).start()
        for j in range(2):
            for i, dz in enumerate((1, 3, 2, 0)):
                remote(
                    piece(turns[j], (depth + dz) % 4),
                    relay.at[j, i] if dz else strips[j].at[col],
                    g_send.at[4 * j + i],
                    s_recv.at[j, i] if dz else g_recv.at[j, col],
                    (pole, row, facing),
                ).start()

    weight_real = table[0, slot[0]]
    weight_imag = table[1, slot[0]]

    def send_all(src, dst, send, recv):
        far = [(dr, ds, dz) for dr in range(ROWS) for ds in range(2) for dz in range(4)]
        far.sort(key=lambda d: -(min(d[0], 4 - d[0]) + d[1] + min(d[2], 4 - d[2])))
        for dr, ds, dz in far[:-1]:
            c = at_depth((side + ds) % 2, dz)
            to = up(dr) * COLS + c
            remote(src.at[to], dst.at[source], send, recv, (pole, up(dr), c)).start()
        dst[source] = src[me]

    @pl.when(active)
    def _():
        count = [0]

        def send_block(r, c, to):
            k = count[0]
            count[0] += 1
            remote(
                block(r, c), block(r, c), l_send.at[k], l_recv.at[r * COLS + c], to
            ).start()

        def send_half(r, c, part, k, to):
            remote(
                half(r, c, part), half(r, c, part), h_send.at[k], h_recv.at[part, c], to
            ).start()

        def wait_block(r, c):
            came(block(r, c), l_recv.at[r * COLS + c])

        def along_rows(c):
            send_block(row, c, (pole, up(1), col))
            send_block(row, c, (pole, up(3), col))

        def pass_on(c):
            k = passed[0]
            passed[0] += 2
            wait_block(up(3), c)
            send_half(up(3), c, 0, k, (pole, up(1), col))
            wait_block(up(1), c)
            send_half(up(1), c, 1, k + 1, (pole, up(3), col))

        def in_plane(c, steps):
            for dz in steps:
                send_block(row, c, (pole, row, at_depth(side, dz)))

        def arrived_in_plane(c):
            wait_block(row, c)
            along_rows(c)

        def forward(j, i):
            came(relay.at[j, i], s_recv.at[j, i])
            remote(
                relay.at[j, i],
                strips[j].at[facing],
                r_send.at[j, i],
                g_recv.at[j, facing],
                (pole, row, at_depth(side, (1, 3, 2)[i])),
            ).start()

        def send_own(j, i):
            send_strip(3 * j + i, j, (depth + (1, 3, 2)[i]) % 4)

        passed = [0]
        order = [col, facing]
        for dz in (1, 3, 2):
            order += [at_depth(side, dz), at_depth(1 - side, dz)]
        in_plane(col, (1, 3))
        along_rows(col)
        send_own(0, 0)
        send_own(0, 1)
        arrived_in_plane(order[2])
        in_plane(col, (2,))
        wait_block(row, facing)
        in_plane(facing, (1, 3, 2))
        along_rows(facing)
        send_own(0, 2)
        arrived_in_plane(order[4])
        forward(0, 0)
        forward(0, 1)
        send_own(1, 0)
        send_own(1, 1)
        for k in (3, 5, 6, 7):
            arrived_in_plane(order[k])
        forward(0, 2)
        send_own(1, 2)
        for k in (0, 1, 2):
            pass_on(order[k])
        forward(1, 0)
        for k in (4, 3):
            pass_on(order[k])
        forward(1, 1)
        for k in (5, 6, 7):
            pass_on(order[k])

        came(owner.at[0], o_recv)
        lane = lax.broadcasted_iota(jnp.int32, (64, 512), 1)
        owner_index = lax.broadcasted_iota(jnp.int32, (64, 512), 0)
        named = ((lane & 127) >> 3) * 4 + (lane >> 7)
        across = lax.broadcasted_iota(jnp.int32, (64, 64), 1)
        down = lax.broadcasted_iota(jnp.int32, (64, 64), 0)
        position = lax.broadcasted_iota(jnp.int32, (1024, 512), 0).astype(F32)
        for s in range(2):
            target = jnp.where(across == down, owner[s].astype(F32), 0.0)
            target = jnp.sum(target, axis=1, keepdims=True).astype(jnp.int32)
            target = ((target & 31) * 32 + (target >> 5) * 8).astype(F32)
            placed = jnp.where(named == owner_index, target, 0.0)
            key = jnp.sum(placed, axis=0, keepdims=True) + (lane[:1] & 7).astype(F32)
            pick[:, s * 512 : (s + 1) * 512] = jnp.where(position == key, 1.0, 0.0).astype(BF)

        forward(1, 2)
        for c in order:
            came(half(up(2), c, 0), h_recv.at[0, c])
            came(half(up(2), c, 1), h_recv.at[1, c])
        for r in range(4):
            for s in range(2):
                b = r * COLS + s * 4 + depth
                before = jnp.int32(0)
                for i in range(NSEL):
                    before += jnp.where(ancestors[0, i] < b, 1, 0)
                before = jnp.minimum(before, NSEL - 1)
                at = (2 * r + s) * BS
                left[:, at : at + BS] = lbuf[before].T

        shares = [None, None]
        columns = []
        for j, rb in enumerate(turns):
            for ds, dz in ((0, 0), (0, 1), (0, 3), (0, 2), (1, 1), (1, 3), (1, 0), (1, 2)):
                c = at_depth((side + ds) % 2, dz)
                if (ds, dz) == (0, 0):
                    own = strips[j].at[c]
                    pltpu.make_async_copy(own, own, local_sem.at[6 * j + 1]).wait()
                else:
                    came(strips[j].at[0], g_recv.at[j, c])
                for part in range(2):
                    for k in range(4):
                        spread[c * 4 + k, part] = strips[j][c, part, :, k * BS : (k + 1) * BS]
            for i in range(NSEL):
                for part in range(2):
                    abuf[part * BS : (part + 1) * BS, i * BS : (i + 1) * BS] = spread[
                        ancestors[0, i], part
                    ]
            acc = jnp.dot(
                abuf[...], lbuf[...].reshape(NSEL * BS, 2 * S), preferred_element_type=F32
            )
            real = acc[:BS, :S] - acc[BS:, S:]
            imag = acc[:BS, S:] + acc[BS:, :S]
            chosen = jnp.int32(0)
            for i in range(NSEL):
                chosen += jnp.where(ancestors[0, i] == row * COLS + rb * 4 + depth, 1, 0)
            keep = lax.broadcast_in_dim(chosen, (BS, S), ()) > 0
            real = jnp.where(keep, real, 0.0)
            imag = jnp.where(keep, imag, 0.0)
            for q in range(4):
                lanes = slice(q * BS, (q + 1) * BS)
                ysend[q, rb] = jnp.concatenate([real[:, lanes], imag[:, lanes]], axis=1).astype(BF)
            for k in (2, 1, 3):
                r = up(k)
                remote(
                    ysend.at[r, rb],
                    yrecv.at[row, rb],
                    y_send.at[j, k],
                    y_recv.at[row, rb],
                    (pole, r, col),
                ).start()
            yrecv[row, rb] = ysend[row, rb]
            target = (column_send, column_out)[j]
            target[:, 0, :] = -real
            target[:, 1, :] = -imag
            if j == 0:
                remote(column_send, column_out, c_send, c_recv, (pole, row, facing)).start()
            share = -(weight_real * imag + weight_imag * real)
            columns.append(
                jnp.concatenate([share[:, q * BS : (q + 1) * BS] for q in range(4)], axis=0)
            )
        first = lax.broadcast_in_dim(works, columns[0].shape, ()) == 1
        share = jnp.concatenate(
            [
                jnp.where(first, columns[0], columns[1]),
                jnp.where(first, columns[1], columns[0]),
            ],
            axis=0,
        )
        high = share.astype(BF)
        low = (share - high.astype(F32)).astype(BF)
        tiles = jnp.dot(
            pick[...], jnp.concatenate([high, low], axis=1), preferred_element_type=F32
        )
        tiles = tiles[:, :BS] + tiles[:, BS:]
        tsend[...] = tiles.astype(BF).reshape(GRID, 32, BS)

        send_all(tsend, trecv, t_send, t_recv)

        for k in (1, 3, 2):
            for rb in range(2):
                came(ysend.at[0, 0], y_recv.at[up(k), rb])
        mixed = jnp.dot(
            left[...], yrecv[...].reshape(8 * BS, 2 * BS), preferred_element_type=F32
        )
        diag_real = mixed[:S, :BS] - mixed[S:, BS:]
        diag_imag = mixed[:S, BS:] + mixed[S:, :BS]
        dsend[...] = (
            jnp.concatenate([diag_real, diag_imag], axis=1)
            .astype(BF)
            .reshape(GRID, S // GRID, 2 * BS)
        )

        send_all(dsend, drecv, d_send, d_recv)

    def arrivals(ref, recv):
        @pl.when(active)
        def _():
            came(ref.at[pl.ds(0, GRID // 2 - 1)], recv)

        @pl.when(jnp.logical_not(active))
        def _():
            came(ref, recv)

    arrivals(trecv, t_recv)
    total = jnp.sum(trecv[...].astype(F32), axis=0)
    psend[...] = total.reshape(POLES, 8, BS)
    pl.semaphore_wait(beside_sem, len(beside))
    for k in range(1, POLES):
        p = (pole + k) % POLES
        remote(psend.at[p], precv.at[pole], p_send.at[k], p_recv.at[pole], (p, row, col)).start()
    precv[pole] = psend[pole]

    arrivals(drecv, d_recv)
    dreal, dimag = [], []
    for q in range(4):
        quarter = jnp.sum(drecv[q * 4 : (q + 1) * 4].astype(F32), axis=0)
        dreal.append(quarter[:, :BS])
        dimag.append(quarter[:, BS:])
    dreal = jnp.concatenate(dreal, axis=1) + dinv[:, 0, :]
    dimag = jnp.concatenate(dimag, axis=1) + dinv[:, 1, :]
    qsend[...] = weight_real * dimag + weight_imag * dreal
    for k in (2, 3, 1):
        p = (pole + k) % POLES
        remote(qsend, qrecv.at[pole], q_send.at[k], q_recv.at[pole], (p, row, col)).start()
    qrecv[pole] = qsend[...]
    diag_out[:, 0, :] = dreal
    diag_out[:, 1, :] = dimag
    for k in range(1, POLES):
        p = (pole + k) % POLES
        came(psend.at[0], p_recv.at[p])
    tile_out[...] = jnp.sum(precv[...], axis=0)

    @pl.when(jnp.logical_not(active))
    def _():
        sent(lbuf.at[0, pl.ds(0, LROWS)], l_send.at[0])
        sent(owner.at[0], o_send)
        for n in range(8):
            sent(first_strips.at[0], g_send.at[n])
        came(column_out, c_recv)

    @pl.when(active)
    def _():
        for n in range(22):
            sent(lbuf.at[0, pl.ds(0, LROWS)], l_send.at[n])
        for n in range(16):
            sent(lbuf.at[0, pl.ds(0, HALF)], h_send.at[n])
        for n in range(6):
            sent(first_strips.at[0], g_send.at[n])
        for j in range(2):
            for i in range(3):
                sent(relay.at[j, i], r_send.at[j, i])
            for k in (1, 2, 3):
                sent(ysend.at[0, 0], y_send.at[j, k])
        sent(column_send, c_send)
        sent(tsend.at[pl.ds(0, GRID - 1)], t_send)
        sent(dsend.at[pl.ds(0, GRID - 1)], d_send)

    for k in range(1, POLES):
        sent(psend.at[0], p_send.at[k])
        sent(qsend, q_send.at[k])
    for k in range(1, POLES):
        p = (pole + k) % POLES
        came(qsend, q_recv.at[p])
    density_out[:, 0, :] = jnp.sum(qrecv[...], axis=0)


def hand_out(*refs):
    done = refs[8]
    copies = [pltpu.make_async_copy(refs[k], refs[4 + k], done.at[k]) for k in range(4)]
    for copy in copies:
        copy.start()
    for copy in copies:
        copy.wait()


def body(inverse, factor, dinv, ancestors, owner, weight_table, pole_slot):
    vmem = pl.BlockSpec(memory_space=pltpu.VMEM)
    hbm = pl.BlockSpec(memory_space=pl.ANY)
    dma = pltpu.SemaphoreType.DMA
    column, diag, density, tile = pl.pallas_call(
        kernel,
        name="supernode",
        out_shape=(
            pltpu.VMEM((BS, 2, S), F32),
            pltpu.VMEM((S // GRID, 2, S), F32),
            pltpu.VMEM((S // GRID, 1, S), F32),
            pltpu.VMEM((8, BS), F32),
        ),
        in_specs=[pl.BlockSpec(memory_space=pltpu.HBM)] * 6 + [pl.BlockSpec(memory_space=pltpu.SMEM)],
        out_specs=(vmem,) * 4,
        scratch_shapes=[
            pltpu.VMEM((NSEL, BS, 2 * S), BF),
            pltpu.VMEM((COLS, 2, BS, S), BF),
            pltpu.VMEM((COLS, 2, BS, S), BF),
            pltpu.VMEM((2, 3, 2, BS, S), BF),
            pltpu.VMEM((COLS * 4, 2, BS, BS), BF),
            pltpu.VMEM((2 * BS, NSEL * BS), BF),
            pltpu.VMEM((2 * S, 8 * BS), BF),
            pltpu.VMEM((BS, 2, S), F32),
            pltpu.VMEM((S // GRID, 2, S), F32),
            pltpu.VMEM((2, 1, 64), jnp.int32),
            pltpu.SMEM((1, NSEL), jnp.int32),
            pltpu.SMEM((2, NWEIGHT), F32),
            pltpu.VMEM((4, 2, BS, 2 * BS), BF),
            pltpu.VMEM((4, 2, BS, 2 * BS), BF),
            pltpu.VMEM((GRID, S // GRID, 2 * BS), BF),
            pltpu.VMEM((GRID // 2, S // GRID, 2 * BS), BF),
            pltpu.VMEM((1024, 1024), BF),
            pltpu.VMEM((GRID, 32, BS), BF),
            pltpu.VMEM((GRID // 2, 32, BS), BF),
            pltpu.VMEM((POLES, 8, BS), F32),
            pltpu.VMEM((POLES, 8, BS), F32),
            pltpu.VMEM((S // GRID, S), F32),
            pltpu.VMEM((POLES, S // GRID, S), F32),
            pltpu.SemaphoreType.REGULAR,
            dma((8,)),
            dma((22,)),
            dma((GRID,)),
            dma((16,)),
            dma((2, COLS)),
            dma((8,)),
            dma((2, COLS)),
            dma((2, 3)),
            dma((2, 3)),
            dma,
            dma,
            dma,
            dma,
            dma((2, 4)),
            dma((4, 2)),
            dma,
            dma,
            dma,
            dma,
            dma((POLES,)),
            dma((POLES,)),
            dma((POLES,)),
            dma((POLES,)),
        ],
        compiler_params=pltpu.CompilerParams(
            collective_id=0, has_side_effects=True, vmem_limit_bytes=56 << 20
        ),
    )(
        *(
            pltpu.with_memory_space_constraint(x, pltpu.HBM)
            for x in (
                inverse.reshape(2, 1024, 512),
                factor.reshape(LROWS, 2 * S),
                dinv.reshape(S // GRID, 2, S),
                ancestors,
                owner.reshape(1, 64),
                weight_table,
            )
        ),
        pole_slot,
    )
    column, diag, density, tile = pl.pallas_call(
        hand_out,
        name="hand_out",
        out_shape=tuple(jax.ShapeDtypeStruct(x.shape, F32) for x in (column, diag, density, tile)),
        in_specs=[vmem] * 4,
        out_specs=(hbm,) * 4,
        scratch_shapes=[dma((4,))],
        compiler_params=pltpu.CompilerParams(vmem_limit_bytes=1 << 20),
    )(column, diag, density, tile)
    return (
        column.reshape(BS, 1, 1, 2, S),
        diag.reshape(S // GRID, 1, 1, 2, S),
        density,
        tile.reshape(1, 8, BS),
    )


def solution(mesh):
    grid = ("row", "col")
    in_specs = (
        P("pole", None, "row", "col"),
        P("pole", None, grid, None),
        P(grid, "pole", None, None, None),
        P(),
        P(grid, None),
        P(),
        P("pole"),
    )
    out_specs = (
        P(grid, "pole", None, None, None),
        P(grid, "pole", None, None, None),
        P(grid, None, None),
        P(("pole", "row", "col"), None, None),
    )
    return jax.shard_map(body, mesh=mesh, in_specs=in_specs, out_specs=out_specs, check_vma=False)
```

```python
import jax
import jax.numpy as jnp
from jax import lax
from jax.experimental import pallas as pl
from jax.experimental.pallas import tpu as pltpu
from jax.sharding import PartitionSpec as P

S = 512
BS = 128
NSEL = 16
NWEIGHT = 16
ROWS = 4
COLS = 8
POLES = 4
GRID = ROWS * COLS
LROWS = NSEL * BS // GRID
HALF = LROWS // 2
MESH = pl.DeviceIdType.MESH
BF = jnp.bfloat16
F32 = jnp.float32


def kernel(
    inverse,
    factor,
    dinv_in,
    ancestors_in,
    owner_in,
    table_in,
    slot,
    column_out,
    diag_out,
    density_out,
    tile_out,
    lbuf,
    first_strips,
    second_strips,
    relay,
    spread,
    abuf,
    left,
    column_send,
    dinv,
    owner,
    ancestors,
    table,
    ysend,
    yrecv,
    dsend,
    drecv,
    pick,
    tsend,
    trecv,
    psend,
    precv,
    qsend,
    qrecv,
    beside_sem,
    local_sem,
    l_send,
    l_recv,
    h_send,
    h_recv,
    g_send,
    g_recv,
    r_send,
    s_recv,
    o_send,
    o_recv,
    c_send,
    c_recv,
    y_send,
    y_recv,
    d_send,
    d_recv,
    t_send,
    t_recv,
    p_send,
    p_recv,
    q_send,
    q_recv,
):
    pole, row, col = lax.axis_index("pole"), lax.axis_index("row"), lax.axis_index("col")
    side, depth = col // 4, col % 4
    me = row * COLS + col
    works = pole % 2
    active = side == works
    facing = (1 - side) * 4 + depth
    source = row * 4 + depth
    turns = (1 - works, works)
    strips = (first_strips, second_strips)

    def at_depth(s, dz):
        return s * 4 + (depth + dz) % 4

    def up(k):
        return (row + k) % ROWS

    def remote(src, dst, send, recv, to):
        return pltpu.make_async_remote_copy(
            src_ref=src,
            dst_ref=dst,
            send_sem=send,
            recv_sem=recv,
            device_id=to,
            device_id_type=MESH,
        )

    here = (pole, row, col)

    def sent(ref, send):
        remote(ref, ref, send, q_recv.at[0], here).wait_send()

    def came(ref, recv):
        remote(ref, ref, q_send.at[0], recv, here).wait_recv()

    own_factor = pltpu.make_async_copy(
        factor, lbuf.at[me // 2, pl.ds((me % 2) * LROWS, LROWS)], local_sem.at[0]
    )
    own_factor.start()
    small = [
        pltpu.make_async_copy(source, target, local_sem.at[2 + n])
        for n, (source, target) in enumerate(
            (
                (owner_in, owner.at[side]),
                (ancestors_in, ancestors),
                (table_in, table),
                (dinv_in, dinv),
            )
        )
    ]
    for copy in small:
        copy.start()

    def piece(rb, z):
        return inverse.at[:, pl.ds((rb * 4 + z) * BS, BS)]

    @pl.when(active)
    def _():
        for j, rb in enumerate(turns):
            pltpu.make_async_copy(
                piece(rb, depth), strips[j].at[col], local_sem.at[6 * j + 1]
            ).start()

    barrier = pltpu.get_barrier_semaphore()
    beside = (((pole + 2) % POLES, row, facing), ((pole + 2) % POLES + 1 - 2 * works, row, facing))
    neighbours = [
        (pole, row, facing),
        (pole, row, at_depth(side, 1)),
        (pole, row, at_depth(side, 3)),
        (pole, up(1), col),
        (pole, up(3), col),
        (pole + 1 - 2 * works, row, col),
        *beside,
    ]
    for device in neighbours:
        pl.semaphore_signal(barrier, inc=1, device_id=device, device_id_type=MESH)
    pl.semaphore_wait(barrier, len(neighbours))
    for device in beside:
        pl.semaphore_signal(beside_sem, inc=1, device_id=device, device_id_type=MESH)
    own_factor.wait()
    for copy in small:
        copy.wait()

    def block(r, c):
        return lbuf.at[r * 4 + c // 2, pl.ds((c % 2) * LROWS, LROWS)]

    def half(r, c, part):
        return lbuf.at[r * 4 + c // 2, pl.ds((c % 2) * LROWS + part * HALF, HALF)]

    def send_strip(n, j, z):
        remote(
            piece(turns[j], z),
            strips[j].at[col],
            g_send.at[n],
            g_recv.at[j, col],
            (pole, row, works * 4 + z),
        ).start()

    @pl.when(jnp.logical_not(active))
    def _():
        remote(
            block(row, col), block(row, col), l_send.at[0], l_recv.at[me], (pole, row, facing)
        ).start()
        remote(owner.at[side], owner.at[side], o_send, o_recv, (pole, row, facing)).start()
        for j in range(2):
            for i, dz in enumerate((1, 3, 2, 0)):
                remote(
                    piece(turns[j], (depth + dz) % 4),
                    relay.at[j, i] if dz else strips[j].at[col],
                    g_send.at[4 * j + i],
                    s_recv.at[j, i] if dz else g_recv.at[j, col],
                    (pole, row, facing),
                ).start()

    weight_real = table[0, slot[0]]
    weight_imag = table[1, slot[0]]

    def send_all(src, dst, send, recv):
        far = [(dr, ds, dz) for dr in range(ROWS) for ds in range(2) for dz in range(4)]
        far.sort(key=lambda d: (-min(d[2], 4 - d[2]), -d[1], -min(d[0], 4 - d[0])))
        for dr, ds, dz in far[:-1]:
            c = at_depth((side + ds) % 2, dz)
            to = up(dr) * COLS + c
            remote(src.at[to], dst.at[source], send, recv, (pole, up(dr), c)).start()
        dst[source] = src[me]

    @pl.when(active)
    def _():
        count = [0]

        def send_block(r, c, to):
            k = count[0]
            count[0] += 1
            remote(
                block(r, c), block(r, c), l_send.at[k], l_recv.at[r * COLS + c], to
            ).start()

        def send_half(r, c, part, k, to):
            remote(
                half(r, c, part), half(r, c, part), h_send.at[k], h_recv.at[part, c], to
            ).start()

        def wait_block(r, c):
            came(block(r, c), l_recv.at[r * COLS + c])

        def along_rows(c):
            send_block(row, c, (pole, up(1), col))
            send_block(row, c, (pole, up(3), col))

        def pass_on(c):
            k = passed[0]
            passed[0] += 2
            wait_block(up(3), c)
            send_half(up(3), c, 0, k, (pole, up(1), col))
            wait_block(up(1), c)
            send_half(up(1), c, 1, k + 1, (pole, up(3), col))

        def in_plane(c, steps):
            for dz in steps:
                send_block(row, c, (pole, row, at_depth(side, dz)))

        def arrived_in_plane(c):
            wait_block(row, c)
            along_rows(c)

        def forward(j, i):
            came(relay.at[j, i], s_recv.at[j, i])
            remote(
                relay.at[j, i],
                strips[j].at[facing],
                r_send.at[j, i],
                g_recv.at[j, facing],
                (pole, row, at_depth(side, (1, 3, 2)[i])),
            ).start()

        def send_own(j, i):
            send_strip(3 * j + i, j, (depth + (1, 3, 2)[i]) % 4)

        passed = [0]
        order = [col, facing]
        for dz in (1, 3, 2):
            order += [at_depth(side, dz), at_depth(1 - side, dz)]
        in_plane(col, (1, 3))
        along_rows(col)
        send_own(0, 0)
        send_own(0, 1)
        arrived_in_plane(order[2])
        in_plane(col, (2,))
        wait_block(row, facing)
        in_plane(facing, (1, 3, 2))
        along_rows(facing)
        send_own(0, 2)
        arrived_in_plane(order[4])
        forward(0, 0)
        forward(0, 1)
        send_own(1, 0)
        send_own(1, 1)
        for k in (3, 5, 6, 7):
            arrived_in_plane(order[k])
        forward(0, 2)
        send_own(1, 2)
        for k in (0, 1, 2):
            pass_on(order[k])
        forward(1, 0)
        for k in (4, 3):
            pass_on(order[k])
        forward(1, 1)
        for k in (5, 6, 7):
            pass_on(order[k])

        came(owner.at[0], o_recv)
        lane = lax.broadcasted_iota(jnp.int32, (64, 512), 1)
        owner_index = lax.broadcasted_iota(jnp.int32, (64, 512), 0)
        named = ((lane & 127) >> 3) * 4 + (lane >> 7)
        across = lax.broadcasted_iota(jnp.int32, (64, 64), 1)
        down = lax.broadcasted_iota(jnp.int32, (64, 64), 0)
        position = lax.broadcasted_iota(jnp.int32, (1024, 512), 0).astype(F32)
        for s in range(2):
            target = jnp.where(across == down, owner[s].astype(F32), 0.0)
            target = jnp.sum(target, axis=1, keepdims=True).astype(jnp.int32)
            target = ((target & 31) * 32 + (target >> 5) * 8).astype(F32)
            placed = jnp.where(named == owner_index, target, 0.0)
            key = jnp.sum(placed, axis=0, keepdims=True) + (lane[:1] & 7).astype(F32)
            pick[:, s * 512 : (s + 1) * 512] = jnp.where(position == key, 1.0, 0.0).astype(BF)

        forward(1, 2)
        for c in order:
            came(half(up(2), c, 0), h_recv.at[0, c])
            came(half(up(2), c, 1), h_recv.at[1, c])
        for r in range(4):
            for s in range(2):
                b = r * COLS + s * 4 + depth
                before = jnp.int32(0)
                for i in range(NSEL):
                    before += jnp.where(ancestors[0, i] < b, 1, 0)
                before = jnp.minimum(before, NSEL - 1)
                at = (2 * r + s) * BS
                left[:, at : at + BS] = lbuf[before].T

        shares = [None, None]
        columns = []
        for j, rb in enumerate(turns):
            for ds, dz in ((0, 0), (0, 1), (0, 3), (0, 2), (1, 1), (1, 3), (1, 0), (1, 2)):
                c = at_depth((side + ds) % 2, dz)
                if (ds, dz) == (0, 0):
                    own = strips[j].at[c]
                    pltpu.make_async_copy(own, own, local_sem.at[6 * j + 1]).wait()
                else:
                    came(strips[j].at[0], g_recv.at[j, c])
                for part in range(2):
                    for k in range(4):
                        spread[c * 4 + k, part] = strips[j][c, part, :, k * BS : (k + 1) * BS]
            for i in range(NSEL):
                for part in range(2):
                    abuf[part * BS : (part + 1) * BS, i * BS : (i + 1) * BS] = spread[
                        ancestors[0, i], part
                    ]
            acc = jnp.dot(
                abuf[...], lbuf[...].reshape(NSEL * BS, 2 * S), preferred_element_type=F32
            )
            real = acc[:BS, :S] - acc[BS:, S:]
            imag = acc[:BS, S:] + acc[BS:, :S]
            chosen = jnp.int32(0)
            for i in range(NSEL):
                chosen += jnp.where(ancestors[0, i] == row * COLS + rb * 4 + depth, 1, 0)
            keep = lax.broadcast_in_dim(chosen, (BS, S), ()) > 0
            real = jnp.where(keep, real, 0.0)
            imag = jnp.where(keep, imag, 0.0)
            for q in range(4):
                lanes = slice(q * BS, (q + 1) * BS)
                ysend[q, rb] = jnp.concatenate([real[:, lanes], imag[:, lanes]], axis=1).astype(BF)
            for k in (2, 1, 3):
                r = up(k)
                remote(
                    ysend.at[r, rb],
                    yrecv.at[row, rb],
                    y_send.at[j, k],
                    y_recv.at[row, rb],
                    (pole, r, col),
                ).start()
            yrecv[row, rb] = ysend[row, rb]
            target = (column_send, column_out)[j]
            target[:, 0, :] = -real
            target[:, 1, :] = -imag
            if j == 0:
                remote(column_send, column_out, c_send, c_recv, (pole, row, facing)).start()
            share = -(weight_real * imag + weight_imag * real)
            columns.append(
                jnp.concatenate([share[:, q * BS : (q + 1) * BS] for q in range(4)], axis=0)
            )
        first = lax.broadcast_in_dim(works, columns[0].shape, ()) == 1
        share = jnp.concatenate(
            [
                jnp.where(first, columns[0], columns[1]),
                jnp.where(first, columns[1], columns[0]),
            ],
            axis=0,
        )
        high = share.astype(BF)
        low = (share - high.astype(F32)).astype(BF)
        tiles = jnp.dot(
            pick[...], jnp.concatenate([high, low], axis=1), preferred_element_type=F32
        )
        tiles = tiles[:, :BS] + tiles[:, BS:]
        tsend[...] = tiles.astype(BF).reshape(GRID, 32, BS)

        send_all(tsend, trecv, t_send, t_recv)

        for k in (1, 3, 2):
            for rb in range(2):
                came(ysend.at[0, 0], y_recv.at[up(k), rb])
        mixed = jnp.dot(
            left[...], yrecv[...].reshape(8 * BS, 2 * BS), preferred_element_type=F32
        )
        diag_real = mixed[:S, :BS] - mixed[S:, BS:]
        diag_imag = mixed[:S, BS:] + mixed[S:, :BS]
        dsend[...] = (
            jnp.concatenate([diag_real, diag_imag], axis=1)
            .astype(BF)
            .reshape(GRID, S // GRID, 2 * BS)
        )

        send_all(dsend, drecv, d_send, d_recv)

    def arrivals(ref, recv):
        @pl.when(active)
        def _():
            came(ref.at[pl.ds(0, GRID // 2 - 1)], recv)

        @pl.when(jnp.logical_not(active))
        def _():
            came(ref, recv)

    arrivals(trecv, t_recv)
    total = jnp.sum(trecv[...].astype(F32), axis=0)
    psend[...] = total.reshape(POLES, 8, BS)
    pl.semaphore_wait(beside_sem, len(beside))
    for k in range(1, POLES):
        p = (pole + k) % POLES
        remote(psend.at[p], precv.at[pole], p_send.at[k], p_recv.at[pole], (p, row, col)).start()
    precv[pole] = psend[pole]

    arrivals(drecv, d_recv)
    dreal, dimag = [], []
    for q in range(4):
        quarter = jnp.sum(drecv[q * 4 : (q + 1) * 4].astype(F32), axis=0)
        dreal.append(quarter[:, :BS])
        dimag.append(quarter[:, BS:])
    dreal = jnp.concatenate(dreal, axis=1) + dinv[:, 0, :]
    dimag = jnp.concatenate(dimag, axis=1) + dinv[:, 1, :]
    qsend[...] = weight_real * dimag + weight_imag * dreal
    for k in range(1, POLES):
        p = (pole + k) % POLES
        remote(qsend, qrecv.at[pole], q_send.at[k], q_recv.at[pole], (p, row, col)).start()
    qrecv[pole] = qsend[...]
    diag_out[:, 0, :] = dreal
    diag_out[:, 1, :] = dimag
    for k in range(1, POLES):
        p = (pole + k) % POLES
        came(psend.at[0], p_recv.at[p])
    tile_out[...] = jnp.sum(precv[...], axis=0)

    @pl.when(jnp.logical_not(active))
    def _():
        sent(lbuf.at[0, pl.ds(0, LROWS)], l_send.at[0])
        sent(owner.at[0], o_send)
        for n in range(8):
            sent(first_strips.at[0], g_send.at[n])
        came(column_out, c_recv)

    @pl.when(active)
    def _():
        for n in range(22):
            sent(lbuf.at[0, pl.ds(0, LROWS)], l_send.at[n])
        for n in range(16):
            sent(lbuf.at[0, pl.ds(0, HALF)], h_send.at[n])
        for n in range(6):
            sent(first_strips.at[0], g_send.at[n])
        for j in range(2):
            for i in range(3):
                sent(relay.at[j, i], r_send.at[j, i])
            for k in (1, 2, 3):
                sent(ysend.at[0, 0], y_send.at[j, k])
        sent(column_send, c_send)
        sent(tsend.at[pl.ds(0, GRID - 1)], t_send)
        sent(dsend.at[pl.ds(0, GRID - 1)], d_send)

    for k in range(1, POLES):
        sent(psend.at[0], p_send.at[k])
        sent(qsend, q_send.at[k])
    for k in range(1, POLES):
        p = (pole + k) % POLES
        came(qsend, q_recv.at[p])
    density_out[:, 0, :] = jnp.sum(qrecv[...], axis=0)


def hand_out(*refs):
    done = refs[8]
    copies = [pltpu.make_async_copy(refs[k], refs[4 + k], done.at[k]) for k in range(4)]
    for copy in copies:
        copy.start()
    for copy in copies:
        copy.wait()


def body(inverse, factor, dinv, ancestors, owner, weight_table, pole_slot):
    vmem = pl.BlockSpec(memory_space=pltpu.VMEM)
    hbm = pl.BlockSpec(memory_space=pl.ANY)
    dma = pltpu.SemaphoreType.DMA
    column, diag, density, tile = pl.pallas_call(
        kernel,
        name="supernode",
        out_shape=(
            pltpu.VMEM((BS, 2, S), F32),
            pltpu.VMEM((S // GRID, 2, S), F32),
            pltpu.VMEM((S // GRID, 1, S), F32),
            pltpu.VMEM((8, BS), F32),
        ),
        in_specs=[pl.BlockSpec(memory_space=pltpu.HBM)] * 6 + [pl.BlockSpec(memory_space=pltpu.SMEM)],
        out_specs=(vmem,) * 4,
        scratch_shapes=[
            pltpu.VMEM((NSEL, BS, 2 * S), BF),
            pltpu.VMEM((COLS, 2, BS, S), BF),
            pltpu.VMEM((COLS, 2, BS, S), BF),
            pltpu.VMEM((2, 3, 2, BS, S), BF),
            pltpu.VMEM((COLS * 4, 2, BS, BS), BF),
            pltpu.VMEM((2 * BS, NSEL * BS), BF),
            pltpu.VMEM((2 * S, 8 * BS), BF),
            pltpu.VMEM((BS, 2, S), F32),
            pltpu.VMEM((S // GRID, 2, S), F32),
            pltpu.VMEM((2, 1, 64), jnp.int32),
            pltpu.SMEM((1, NSEL), jnp.int32),
            pltpu.SMEM((2, NWEIGHT), F32),
            pltpu.VMEM((4, 2, BS, 2 * BS), BF),
            pltpu.VMEM((4, 2, BS, 2 * BS), BF),
            pltpu.VMEM((GRID, S // GRID, 2 * BS), BF),
            pltpu.VMEM((GRID // 2, S // GRID, 2 * BS), BF),
            pltpu.VMEM((1024, 1024), BF),
            pltpu.VMEM((GRID, 32, BS), BF),
            pltpu.VMEM((GRID // 2, 32, BS), BF),
            pltpu.VMEM((POLES, 8, BS), F32),
            pltpu.VMEM((POLES, 8, BS), F32),
            pltpu.VMEM((S // GRID, S), F32),
            pltpu.VMEM((POLES, S // GRID, S), F32),
            pltpu.SemaphoreType.REGULAR,
            dma((8,)),
            dma((22,)),
            dma((GRID,)),
            dma((16,)),
            dma((2, COLS)),
            dma((8,)),
            dma((2, COLS)),
            dma((2, 3)),
            dma((2, 3)),
            dma,
            dma,
            dma,
            dma,
            dma((2, 4)),
            dma((4, 2)),
            dma,
            dma,
            dma,
            dma,
            dma((POLES,)),
            dma((POLES,)),
            dma((POLES,)),
            dma((POLES,)),
        ],
        compiler_params=pltpu.CompilerParams(
            collective_id=0, has_side_effects=True, vmem_limit_bytes=56 << 20
        ),
    )(
        *(
            pltpu.with_memory_space_constraint(x, pltpu.HBM)
            for x in (
                inverse.reshape(2, 1024, 512),
                factor.reshape(LROWS, 2 * S),
                dinv.reshape(S // GRID, 2, S),
                ancestors,
                owner.reshape(1, 64),
                weight_table,
            )
        ),
        pole_slot,
    )
    column, diag, density, tile = pl.pallas_call(
        hand_out,
        name="hand_out",
        out_shape=tuple(jax.ShapeDtypeStruct(x.shape, F32) for x in (column, diag, density, tile)),
        in_specs=[vmem] * 4,
        out_specs=(hbm,) * 4,
        scratch_shapes=[dma((4,))],
        compiler_params=pltpu.CompilerParams(vmem_limit_bytes=1 << 20),
    )(column, diag, density, tile)
    return (
        column.reshape(BS, 1, 1, 2, S),
        diag.reshape(S // GRID, 1, 1, 2, S),
        density,
        tile.reshape(1, 8, BS),
    )


def solution(mesh):
    grid = ("row", "col")
    in_specs = (
        P("pole", None, "row", "col"),
        P("pole", None, grid, None),
        P(grid, "pole", None, None, None),
        P(),
        P(grid, None),
        P(),
        P("pole"),
    )
    out_specs = (
        P(grid, "pole", None, None, None),
        P(grid, "pole", None, None, None),
        P(grid, None, None),
        P(("pole", "row", "col"), None, None),
    )
    return jax.shard_map(body, mesh=mesh, in_specs=in_specs, out_specs=out_specs, check_vma=False)
```
